512 devices in a mesh: section: 4 (over x), ctx: 64 (over y, z), mp: 2 (over core).
Axes of the slice: x: 4, y: 8, z: 8, core: 2. Of those that a mesh axis runs over, the one named last changes fastest.
Arguments:
- head_input: bfloat16 [4, 16384, 2048], P('section', 'ctx', 'mp'), may hold values from -6 to 6
- state_proj: bfloat16 [4, 16384, 256], P('section', 'ctx'), may hold values from -6 to 6
- gate_input: bfloat16 [4, 16384, 2048], P('section', 'ctx', 'mp'), may hold values from -6 to 6
- step_raw: float32 [4, 32, 16384], P('section', 'mp', 'ctx'), may hold values from -2 to 2
- step_bias: float32 [4, 32], P('section', 'mp'), may hold values from -9.5 to -3
- decay_log: float32 [4, 32], P('section', 'mp'), may hold values from -7 to 1.5
- skip_gain: float32 [4, 32], P('section', 'mp'), may hold values from 0.5 to 1.5
- conv_head: float32 [4, 4, 2048], P('section', None, 'mp'), may hold values from -3 to 3
- conv_state: float32 [4, 4, 256], P('section'), may hold values from -3 to 3
- norm_gain: float32 [4, 2048], P('section', 'mp'), may hold values from 0.1 to 1.9
- next_weight: bfloat16 [4, 2048, 4096], P('section', 'ctx', 'mp'), may hold values from -0.125 to 0.125
Outputs:
- projected: bfloat16 [4, 16384, 4096], P('section', 'ctx', 'mp')
The draws below stay inside these ranges and needn't reach their ends.
All inputs are finite; a program needn't handle non-finite values.
Results may differ from the reference program's by a relative error of at most 0.0087.
Values may be sent and summed in bfloat16 or wider, within the bound.
No kernel may reach another device: no remote copies, remote signals or barrier semaphores. Data moves between devices by JAX's collectives and lax.ppermute only.
A program may use at most 64 MiB of HBM per device.

```python
import jax
import jax.numpy as jnp
from jax import lax

HEADS = 32
HEAD_DIM = 64
STATE = 128
BLOCK = 256
CONV_TAPS = 4
MODEL_WIDTH = 4096
TOK_DEV = 256
FEATURES = 2048
LENGTH = 16384
SECTIONS = 4


def head_law(key):
    base = jax.random.fold_in(key, 29)
    flag_key, rate_key, size_key = jax.random.split(base, 3)
    fast_share = 0.5
    fast = jax.random.uniform(flag_key, (SECTIONS, HEADS), jnp.float32) < fast_share
    rate_unit = jax.random.uniform(rate_key, (SECTIONS, HEADS), jnp.float32)
    size_unit = jax.random.uniform(size_key, (SECTIONS, HEADS), jnp.float32)
    fast_rate = 0.02 * jnp.exp(rate_unit * jnp.log(2.0))
    slow_rate = 0.3 / LENGTH * jnp.exp(rate_unit * jnp.log(1.0 / 0.3))
    fast_size = 0.015 * jnp.exp(size_unit * jnp.log(0.04 / 0.015))
    slow_size = 0.5 / (7.0 * jnp.sqrt(1.0 * LENGTH)) * jnp.exp(size_unit * jnp.log(4.0))
    rate = jnp.where(fast, fast_rate, slow_rate)
    size = jnp.where(fast, fast_size, slow_size)
    return (rate, size)


def draw_decay_log(key, part):
    rate, size = head_law(key)
    return jnp.log(rate / size).astype(jnp.float32)


def draw_step_bias(key, part):
    rate, size = head_law(key)
    return jnp.log(jnp.expm1(size)).astype(jnp.float32)


def draw_step_raw(key, part):
    block_key, noise_key = jax.random.split(jax.random.fold_in(key, 31))
    block_total = LENGTH // TOK_DEV
    offsets = jax.random.uniform(block_key, (SECTIONS, HEADS, block_total), jnp.float32, minval=-0.7, maxval=0.7)
    noise = 0.4 * jax.random.truncated_normal(noise_key, -3.0, 3.0, (SECTIONS, HEADS, LENGTH), jnp.float32)
    return (noise + jnp.repeat(offsets, TOK_DEV, axis=2)).astype(jnp.float32)


def block_scale(key, dims, cuts, low, top_value):
    def one(dim, shards_of):
        heights = jax.random.uniform(jax.random.fold_in(jax.random.fold_in(key, 6), dim), (shards_of,), jnp.float32, low / len(cuts), top_value / len(cuts))
        return jnp.repeat(jnp.exp(heights), dims[dim] // shards_of).reshape((-1,) + (1,) * (len(dims) - dim - 1))

    loudness = one(*cuts[0])
    for cut in cuts[1:]:
        loudness = loudness * one(*cut)
    return loudness


def scatter_about(key, shape, width, limit, cuts=(), kind=jnp.bfloat16):
    entries = jax.random.normal(key, shape, jnp.float32) * width
    if len(cuts) > 0:
        entries = block_scale(key, shape, cuts, -0.22, 0.18) * entries
    return jnp.clip(entries, min=-limit, max=limit).astype(kind)


def setup_inputs(seed: int = 0) -> dict:
    key_of = jax.random.split(jax.random.key(seed), 12)
    head_input = scatter_about(key_of[0], (SECTIONS, LENGTH, FEATURES), 1.0, 6.0, ((0, 4), (1, 64), (2, 2)))
    state_proj = scatter_about(key_of[1], (SECTIONS, LENGTH, 2 * STATE), 1.0, 6.0, ((0, 4), (1, 64)))
    gate_input = scatter_about(key_of[2], (SECTIONS, LENGTH, FEATURES), 1.0, 6.0, ((0, 4), (1, 64), (2, 2)))
    step_raw = draw_step_raw(jax.random.fold_in(key_of[11], 71), 0)
    step_bias = draw_step_bias(jax.random.fold_in(key_of[11], 71), 0)
    decay_log = draw_decay_log(jax.random.fold_in(key_of[11], 71), 0)
    skip_gain = jnp.clip(0.5 + 1.0 * jax.random.uniform(key_of[6], (SECTIONS, HEADS), jnp.float32) ** block_scale(key_of[6], (SECTIONS, HEADS), ((0, 4), (1, 2)), -0.2, 0.2), 0.5, 1.5)
    conv_head = scatter_about(key_of[7], (SECTIONS, CONV_TAPS, FEATURES), CONV_TAPS ** -0.5, 3.0, ((0, 4), (2, 2)), jnp.float32)
    conv_state = scatter_about(key_of[8], (SECTIONS, CONV_TAPS, 2 * STATE), CONV_TAPS ** -0.5, 3.0, ((0, 4),), jnp.float32)
    norm_gain = jnp.clip(1.0 + 0.18 * jax.random.normal(key_of[9], (SECTIONS, FEATURES), jnp.float32), 0.1, 1.9)
    next_weight = scatter_about(key_of[10], (SECTIONS, FEATURES, MODEL_WIDTH), FEATURES ** -0.5, 0.125, ((0, 4), (1, 64), (2, 2)))
    return dict(head_input=head_input, state_proj=state_proj, gate_input=gate_input, step_raw=step_raw, step_bias=step_bias, decay_log=decay_log, skip_gain=skip_gain, conv_head=conv_head, conv_state=conv_state, norm_gain=norm_gain, next_weight=next_weight)


NORM_FLOOR = 0.25
HIGHEST = lax.Precision.HIGHEST

def causal_conv(sequence, weights):
    length = sequence.shape[0]
    padding = jnp.zeros((weights.shape[0] - 1, sequence.shape[1]), sequence.dtype)
    padded = jnp.concatenate([padding, sequence], axis=0).astype(jnp.float32)
    summed = jnp.zeros(sequence.shape, jnp.float32)
    for offset in range(weights.shape[0]):
        summed = summed + weights[offset] * padded[offset:offset + length]
    return summed

def mixer(head_input, state_proj, gate_input, step_raw, step_bias, decay_log, skip_gain, conv_head, conv_state, norm_gain):
    conv_x = jax.nn.silu(causal_conv(head_input, conv_head)).astype(jnp.bfloat16)
    conv_bc = causal_conv(state_proj, conv_state).astype(jnp.bfloat16)
    block_count = LENGTH // BLOCK
    blocks_x = conv_x.reshape(block_count, BLOCK, HEADS, HEAD_DIM)
    blocks_b = conv_bc[:, :STATE].reshape(block_count, BLOCK, STATE)
    blocks_c = conv_bc[:, STATE:].reshape(block_count, BLOCK, STATE)
    step_size = jax.nn.softplus(step_raw + step_bias[:, None])
    log_decay = -jnp.exp(decay_log)[:, None] * step_size
    blocks_step = step_size.reshape(HEADS, block_count, BLOCK).transpose(1, 0, 2)
    blocks_decay = log_decay.reshape(HEADS, block_count, BLOCK).transpose(1, 0, 2)
    row_index = lax.broadcasted_iota(jnp.int32, (BLOCK, BLOCK), 0)
    col_index = lax.broadcasted_iota(jnp.int32, (BLOCK, BLOCK), 1)
    causal_mask = row_index >= col_index

    def block_step(carried, block_items):
        part_x, part_b, part_c, part_step, part_decay = block_items
        cumulative = jnp.cumsum(part_decay, axis=1)
        scores = jnp.dot(part_c, part_b.T, preferred_element_type=jnp.float32)
        decay_diff = jnp.where(causal_mask, cumulative[:, :, None] - cumulative[:, None, :], 0.0)
        mix_weight = jnp.where(causal_mask, scores[None] * jnp.exp(decay_diff) * part_step[:, None, :], 0.0).astype(jnp.bfloat16)
        intra_part = jnp.einsum('hts,shp->thp', mix_weight.astype(jnp.float32), part_x.astype(jnp.float32), precision=HIGHEST)
        tail_weight = jnp.exp(cumulative[:, -1:] - cumulative) * part_step
        weighted_b = (part_b.astype(jnp.float32)[None] * tail_weight[:, :, None]).astype(jnp.bfloat16)
        update = jnp.einsum('shp,hsn->hpn', part_x.astype(jnp.float32), weighted_b.astype(jnp.float32), precision=HIGHEST)
        inter_part = jnp.einsum('tn,hpn->thp', part_c.astype(jnp.float32), carried, precision=HIGHEST) * jnp.exp(cumulative).T[:, :, None]
        output = intra_part + inter_part + skip_gain[None, :, None] * part_x.astype(jnp.float32)
        next_carried = jnp.exp(cumulative[:, -1])[:, None, None] * carried + update
        return (next_carried, output)
    start_state = jnp.zeros((HEADS, HEAD_DIM, STATE), jnp.float32)
    last_state, outputs = lax.scan(block_step, start_state, (blocks_x, blocks_b, blocks_c, blocks_step, blocks_decay))
    mixer_y = outputs.reshape(LENGTH, FEATURES)
    gated = mixer_y * jax.nn.silu(gate_input.astype(jnp.float32))
    mean_square = lax.optimization_barrier(jnp.sum(gated * gated, axis=1)) / FEATURES
    return (gated * lax.rsqrt(mean_square + NORM_FLOOR)[:, None] * norm_gain[None]).astype(jnp.bfloat16)

def reference(head_input, state_proj, gate_input, step_raw, step_bias, decay_log, skip_gain, conv_head, conv_state, norm_gain, next_weight):
    normed_all = []
    for section_index in range(SECTIONS):
        normed_all.append(mixer(head_input[section_index], state_proj[section_index], gate_input[section_index], step_raw[section_index], step_bias[section_index], decay_log[section_index], skip_gain[section_index], conv_head[section_index], conv_state[section_index], norm_gain[section_index]))
    projected = []
    for section_index in range(SECTIONS):
        source = normed_all[(section_index - 1) % SECTIONS]
        projected.append(jnp.dot(source, next_weight[section_index], preferred_element_type=jnp.float32).astype(jnp.bfloat16))
    return jnp.stack(projected)
```

```python
import jax
import jax.numpy as jnp
from jax import lax
from jax.experimental import pallas as pl
from jax.experimental.pallas import tpu as pltpu
from jax.sharding import Mesh
from jax.sharding import PartitionSpec as P

STATE = 128
BLOCK = 256
FEATURES = 2048
CTX = ("ctx_0", "ctx_1")


NORM_FLOOR = 0.25
HIGHEST = lax.Precision.HIGHEST


def from_behind(value, axis, steps):
    count = lax.axis_size(axis)
    first, last = (max(0, -steps), min(count, count - steps))
    return lax.ppermute(value, axis, [(source, source + steps) for source in range(first, last)])


def split_in_two(x):
    high = lax.reduce_precision(x, 8, 7)
    return high.astype(jnp.bfloat16), (x - high).astype(jnp.bfloat16)


def scan_kernel(pieces_ref, prior_ref):
    count, _, width = pieces_ref.shape
    rows = prior_ref.shape[1]
    carried = jnp.zeros((rows, width), jnp.float32)
    for k in range(count):
        prior_ref[k] = carried.astype(jnp.bfloat16)
        factor = pieces_ref[k, rows : rows + 2, :].astype(jnp.float32)
        carried = (factor[0:1] + factor[1:2]) * carried + pieces_ref[k, 0:rows, :].astype(
            jnp.float32
        )


def states_before(state, total_log, axes):
    count = lax.axis_size(axes)
    head_count, head_width, width = state.shape
    rows = head_count * head_width // count
    slices = state.astype(jnp.bfloat16).reshape(count, rows, width)
    high, low = split_in_two(jnp.exp(total_log))
    factors = jnp.stack([high, low], axis=1)
    factors = jnp.repeat(factors, count // head_count, axis=0)
    factors = jnp.broadcast_to(factors[:, :, None], (count, 2, width))
    sent = jnp.concatenate([slices, factors], axis=1)
    pieces = lax.all_to_all(sent, axes, 0, 0, tiled=True)
    prior = pl.pallas_call(
        scan_kernel,
        out_shape=jax.ShapeDtypeStruct((count, rows, width), jnp.bfloat16),
        in_specs=[pl.BlockSpec(memory_space=pltpu.VMEM)],
        out_specs=pl.BlockSpec(memory_space=pltpu.VMEM),
        cost_estimate=pl.CostEstimate(
            flops=3 * count * rows * width, bytes_accessed=4 * count * rows * width, transcendentals=0
        ),
    )(pieces)
    back = lax.all_to_all(prior, axes, 0, 0, tiled=True)
    return back.reshape(head_count, head_width, width)


def other_half(x, axis):
    return lax.ppermute(x, axis, [(0, 1), (1, 0)])


def gathered_total(x, axis):
    return lax.all_gather(x, axis).sum(0)


def shifted(value, axis, steps):
    count = lax.axis_size(axis)
    pairs = [(source, (source + steps) % count) for source in range(count)]
    return lax.ppermute(value, axis, pairs)


def causal_conv(sequence, previous, weights):
    length = sequence.shape[0]
    padded = jnp.concatenate([previous, sequence], axis=0).astype(jnp.float32)
    summed = jnp.zeros(sequence.shape, jnp.float32)
    for offset in range(weights.shape[0]):
        summed = summed + weights[offset] * padded[offset : offset + length]
    return summed


def shards(
    head_input,
    state_proj,
    gate_input,
    step_raw,
    step_bias,
    decay_log,
    skip_gain,
    conv_head,
    conv_state,
    norm_gain,
    next_weight,
):
    full_weight = lax.all_gather(next_weight[0], CTX, axis=0, tiled=True)
    tap_count = conv_head.shape[1]
    token_count = head_input.shape[1]
    local_width = head_input.shape[2]
    head_count = step_raw.shape[1]
    head_width = local_width // head_count
    block_count = token_count // BLOCK
    tails = jnp.concatenate(
        [
            head_input[0, token_count - tap_count + 1 :],
            state_proj[0, token_count - tap_count + 1 :],
        ],
        axis=1,
    )
    previous = from_behind(tails, CTX, 1)
    conv_x = jax.nn.silu(
        causal_conv(head_input[0], previous[:, :local_width], conv_head[0])
    ).astype(jnp.bfloat16)
    conv_bc = causal_conv(state_proj[0], previous[:, local_width:], conv_state[0]).astype(
        jnp.bfloat16
    )
    blocks_x = conv_x.reshape(block_count, BLOCK, head_count, head_width)
    blocks_b = conv_bc[:, :STATE].reshape(block_count, BLOCK, STATE)
    blocks_c = conv_bc[:, STATE:].reshape(block_count, BLOCK, STATE)
    step_size = jax.nn.softplus(step_raw[0] + step_bias[0][:, None])
    log_decay = -jnp.exp(decay_log[0])[:, None] * step_size
    blocks_step = step_size.reshape(head_count, block_count, BLOCK)
    blocks_decay = log_decay.reshape(head_count, block_count, BLOCK)
    row_index = lax.broadcasted_iota(jnp.int32, (BLOCK, BLOCK), 0)
    col_index = lax.broadcasted_iota(jnp.int32, (BLOCK, BLOCK), 1)
    causal_mask = row_index >= col_index
    lower_tri = causal_mask.astype(jnp.float32)
    cumulative = jnp.einsum("hcs,ts->hct", blocks_decay, lower_tri, precision=HIGHEST)
    scores = jnp.einsum("ctn,csn->cts", blocks_c, blocks_b, preferred_element_type=jnp.float32)
    decay_diff = jnp.where(causal_mask, cumulative[..., :, None] - cumulative[..., None, :], 0.0)
    mix_weight = jnp.where(
        causal_mask, scores[None] * jnp.exp(decay_diff) * blocks_step[:, :, None, :], 0.0
    ).astype(jnp.bfloat16)
    intra_part = jnp.einsum(
        "hcts,cshp->cthp", mix_weight, blocks_x, preferred_element_type=jnp.float32
    )
    tail_weight = jnp.exp(cumulative[..., -1:] - cumulative) * blocks_step
    weighted_b = (blocks_b.astype(jnp.float32)[None] * tail_weight[..., None]).astype(jnp.bfloat16)
    updates = jnp.einsum(
        "cshp,hcsn->chpn", blocks_x, weighted_b, preferred_element_type=jnp.float32
    )
    prior_state = states_before(updates[0], cumulative[:, 0, -1], CTX)
    inter_part = (
        jnp.einsum("ctn,hpn->cthp", blocks_c, prior_state, preferred_element_type=jnp.float32)
        * jnp.exp(cumulative).transpose(1, 2, 0)[..., None]
    )
    output = (
        intra_part + inter_part + skip_gain[0][None, None, :, None] * blocks_x.astype(jnp.float32)
    )
    gated = output.reshape(token_count, local_width) * jax.nn.silu(
        gate_input[0].astype(jnp.float32)
    )
    squares = gathered_total(jnp.sum(gated * gated, axis=1), "mp")
    mean_square = squares / FEATURES
    normed = (gated * lax.rsqrt(mean_square + NORM_FLOOR)[:, None] * norm_gain[0][None]).astype(
        jnp.bfloat16
    )
    arrived = shifted(normed, "section", 1)
    other = other_half(arrived, "mp")
    low = lax.axis_index("mp") == 0
    features = jnp.concatenate(
        [jnp.where(low, arrived, other), jnp.where(low, other, arrived)], axis=1
    )
    result = jnp.dot(features, full_weight, preferred_element_type=jnp.float32)
    return result.astype(jnp.bfloat16)[None]


def solution(mesh):
    finer = Mesh(
        mesh.devices.reshape(mesh.shape["section"], 8, 8, mesh.shape["mp"]),
        ("section", "ctx_0", "ctx_1", "mp"),
    )
    in_specs = (
        P("section", CTX, "mp"),
        P("section", CTX, None),
        P("section", CTX, "mp"),
        P("section", "mp", CTX),
        P("section", "mp"),
        P("section", "mp"),
        P("section", "mp"),
        P("section", None, "mp"),
        P("section", None, None),
        P("section", "mp"),
        P("section", CTX, "mp"),
    )
    out_specs = P("section", CTX, "mp")
    return jax.shard_map(
        shards, mesh=finer, in_specs=in_specs, out_specs=out_specs, check_vma=False
    )
```

```python
import jax
import numpy as np
import jax.numpy as jnp
from jax import lax
from jax.experimental import pallas as pl
from jax.experimental.pallas import tpu as pltpu
from jax.sharding import Mesh
from jax.sharding import PartitionSpec as P

STATE = 128
BLOCK = 256
FEATURES = 2048
CTX = ("ctx_0", "ctx_1")


NORM_FLOOR = 0.25
HIGHEST = lax.Precision.HIGHEST


def from_behind(value, axis, steps):
    count = lax.axis_size(axis)
    first, last = (max(0, -steps), min(count, count - steps))
    return lax.ppermute(value, axis, [(source, source + steps) for source in range(first, last)])


def split_in_two(x):
    high = lax.reduce_precision(x, 8, 7)
    return high.astype(jnp.bfloat16), (x - high).astype(jnp.bfloat16)


def scan_kernel(pieces_ref, prior_ref):
    count, _, width = pieces_ref.shape
    rows = prior_ref.shape[1]
    carried = jnp.zeros((rows, width), jnp.float32)
    for k in range(count):
        prior_ref[k] = carried.astype(jnp.bfloat16)
        factor = pieces_ref[k, rows : rows + 2, :].astype(jnp.float32)
        carried = (factor[0:1] + factor[1:2]) * carried + pieces_ref[k, 0:rows, :].astype(
            jnp.float32
        )


def state_slices(state, total_log, axes):
    count = lax.axis_size(axes)
    head_count, head_width, width = state.shape
    rows = head_count * head_width // count
    slices = state.astype(jnp.bfloat16).reshape(count, rows, width)
    high, low = split_in_two(jnp.exp(total_log))
    factors = jnp.stack([high, low], axis=1)
    factors = jnp.repeat(factors, count // head_count, axis=0)
    factors = jnp.broadcast_to(factors[:, :, None], (count, 2, width))
    return jnp.concatenate([slices, factors], axis=1)


def states_before(sent, axes):
    count, rows, width = sent.shape
    rows = rows - 2
    pieces = lax.all_to_all(sent, axes, 0, 0, tiled=True)
    prior = pl.pallas_call(
        scan_kernel,
        out_shape=jax.ShapeDtypeStruct((count, rows, width), jnp.bfloat16),
        in_specs=[pl.BlockSpec(memory_space=pltpu.VMEM)],
        out_specs=pl.BlockSpec(memory_space=pltpu.VMEM),
        cost_estimate=pl.CostEstimate(
            flops=3 * count * rows * width, bytes_accessed=4 * count * rows * width, transcendentals=0
        ),
    )(pieces)
    back = lax.all_to_all(prior, axes, 0, 0, tiled=True)
    return back.reshape(count * rows, width)


ALL_AXES = ("section", *CTX, "mp")


def crossed_groups(first):
    sizes = [lax.axis_size(name) for name in ALL_AXES]
    index = np.arange(np.prod(sizes)).reshape(sizes)
    groups = []
    for section in range(sizes[0]):
        for core in range(2):
            grid = index[section, :, :, core]
            groups += (grid if (core == 0) == first else grid.T).tolist()
    return groups


def weight_part(rows):
    count = lax.axis_size(CTX[0])
    pieces = lax.all_to_all(
        jnp.broadcast_to(rows[None], (count, *rows.shape)),
        ALL_AXES,
        0,
        0,
        axis_index_groups=crossed_groups(True),
        tiled=True,
    )
    return pieces.reshape(count * rows.shape[0], rows.shape[1])


def gathered_weight(part):
    return lax.all_gather(
        part, ALL_AXES, axis_index_groups=crossed_groups(False), axis=0, tiled=True
    )


def weight_order(features):
    tokens, width = features.shape
    outer, inner = (lax.axis_size(name) for name in CTX)
    crossed = features.reshape(tokens, outer, inner, -1).transpose(0, 2, 1, 3)
    return jnp.where(lax.axis_index("mp") == 0, features, crossed.reshape(tokens, width))


def other_half(x, axis):
    return lax.ppermute(x, axis, [(0, 1), (1, 0)])


def gathered_total(x, axis):
    return lax.all_gather(x, axis).sum(0)


def shifted(value, axis, steps):
    count = lax.axis_size(axis)
    pairs = [(source, (source + steps) % count) for source in range(count)]
    return lax.ppermute(value, axis, pairs)


def causal_conv(sequence, previous, weights):
    length = sequence.shape[0]
    padded = jnp.concatenate([previous, sequence], axis=0).astype(jnp.float32)
    summed = jnp.zeros(sequence.shape, jnp.float32)
    for offset in range(weights.shape[0]):
        summed = summed + weights[offset] * padded[offset : offset + length]
    return summed


def shards(
    head_input,
    state_proj,
    gate_input,
    step_raw,
    step_bias,
    decay_log,
    skip_gain,
    conv_head,
    conv_state,
    norm_gain,
    next_weight,
):
    part = weight_part(next_weight[0])
    tap_count = conv_head.shape[1]
    token_count = head_input.shape[1]
    local_width = head_input.shape[2]
    head_count = step_raw.shape[1]
    head_width = local_width // head_count
    block_count = token_count // BLOCK
    tails = jnp.concatenate(
        [
            head_input[0, token_count - tap_count + 1 :],
            state_proj[0, token_count - tap_count + 1 :],
        ],
        axis=1,
    )
    previous = from_behind(tails, CTX, 1)
    conv_x = jax.nn.silu(
        causal_conv(head_input[0], previous[:, :local_width], conv_head[0])
    ).astype(jnp.bfloat16)
    conv_bc = causal_conv(state_proj[0], previous[:, local_width:], conv_state[0]).astype(
        jnp.bfloat16
    )
    blocks_x = conv_x.reshape(block_count, BLOCK, head_count, head_width)
    blocks_b = conv_bc[:, :STATE].reshape(block_count, BLOCK, STATE)
    blocks_c = conv_bc[:, STATE:].reshape(block_count, BLOCK, STATE)
    step_size = jax.nn.softplus(step_raw[0] + step_bias[0][:, None])
    log_decay = -jnp.exp(decay_log[0])[:, None] * step_size
    blocks_step = step_size.reshape(head_count, block_count, BLOCK)
    blocks_decay = log_decay.reshape(head_count, block_count, BLOCK)
    row_index = lax.broadcasted_iota(jnp.int32, (BLOCK, BLOCK), 0)
    col_index = lax.broadcasted_iota(jnp.int32, (BLOCK, BLOCK), 1)
    causal_mask = row_index >= col_index
    lower_tri = causal_mask.astype(jnp.float32)
    cumulative = jnp.einsum("hcs,ts->hct", blocks_decay, lower_tri, precision=HIGHEST)
    scores = jnp.einsum("ctn,csn->cts", blocks_c, blocks_b, preferred_element_type=jnp.float32)
    decay_diff = jnp.where(causal_mask, cumulative[..., :, None] - cumulative[..., None, :], 0.0)
    mix_weight = jnp.where(
        causal_mask, scores[None] * jnp.exp(decay_diff) * blocks_step[:, :, None, :], 0.0
    ).astype(jnp.bfloat16)
    intra_part = jnp.einsum(
        "hcts,cshp->cthp", mix_weight, blocks_x, preferred_element_type=jnp.float32
    )
    tail_weight = jnp.exp(cumulative[..., -1:] - cumulative) * blocks_step
    weighted_b = (blocks_b.astype(jnp.float32)[None] * tail_weight[..., None]).astype(jnp.bfloat16)
    updates = jnp.einsum(
        "cshp,hcsn->chpn", blocks_x, weighted_b, preferred_element_type=jnp.float32
    )
    sent = state_slices(updates[0], cumulative[:, 0, -1], CTX)
    full_weight = gathered_weight(lax.optimization_barrier((part, sent))[0])
    prior_state = states_before(sent, CTX).reshape(head_count, head_width, STATE)
    inter_part = (
        jnp.einsum("ctn,hpn->cthp", blocks_c, prior_state, preferred_element_type=jnp.float32)
        * jnp.exp(cumulative).transpose(1, 2, 0)[..., None]
    )
    output = (
        intra_part + inter_part + skip_gain[0][None, None, :, None] * blocks_x.astype(jnp.float32)
    )
    gated = output.reshape(token_count, local_width) * jax.nn.silu(
        gate_input[0].astype(jnp.float32)
    )
    squares = gathered_total(jnp.sum(gated * gated, axis=1), "mp")
    mean_square = squares / FEATURES
    normed = (gated * lax.rsqrt(mean_square + NORM_FLOOR)[:, None] * norm_gain[0][None]).astype(
        jnp.bfloat16
    )
    arrived = shifted(normed, "section", 1)
    other = other_half(arrived, "mp")
    low = lax.axis_index("mp") == 0
    features = jnp.concatenate(
        [jnp.where(low, arrived, other), jnp.where(low, other, arrived)], axis=1
    )
    result = jnp.dot(weight_order(features), full_weight, preferred_element_type=jnp.float32)
    return result.astype(jnp.bfloat16)[None]


def solution(mesh):
    finer = Mesh(
        mesh.devices.reshape(mesh.shape["section"], 8, 8, mesh.shape["mp"]),
        ("section", "ctx_0", "ctx_1", "mp"),
    )
    in_specs = (
        P("section", CTX, "mp"),
        P("section", CTX, None),
        P("section", CTX, "mp"),
        P("section", "mp", CTX),
        P("section", "mp"),
        P("section", "mp"),
        P("section", "mp"),
        P("section", None, "mp"),
        P("section", None, None),
        P("section", "mp"),
        P("section", CTX, "mp"),
    )
    out_specs = P("section", CTX, "mp")
    return jax.shard_map(
        shards, mesh=finer, in_specs=in_specs, out_specs=out_specs, check_vma=False
    )
```

```python
import jax
import numpy as np
import jax.numpy as jnp
from jax import lax
from jax.experimental import pallas as pl
from jax.experimental.pallas import tpu as pltpu
from jax.sharding import Mesh
from jax.sharding import PartitionSpec as P

STATE = 128
BLOCK = 256
FEATURES = 2048
CTX = ("ctx_0", "ctx_1")
CTX_SIDE = 8
EXTRA = 8
TAIL = 8


NORM_FLOOR = 0.25


def small_vmem(mebibytes):
    return pltpu.CompilerParams(vmem_limit_bytes=mebibytes * 2**20)


HIGHEST = lax.Precision.HIGHEST


def from_behind(value, axis, steps):
    count = lax.axis_size(axis)
    first, last = (max(0, -steps), min(count, count - steps))
    return lax.ppermute(value, axis, [(source, source + steps) for source in range(first, last)])


def split_in_two(x):
    high = lax.reduce_precision(x, 8, 7)
    return high.astype(jnp.bfloat16), (x - high).astype(jnp.bfloat16)


def scan_kernel(pieces_ref, prior_ref):
    count, _, width = pieces_ref.shape
    rows = prior_ref.shape[1]
    carried = jnp.zeros((rows, width), jnp.float32)
    for k in range(count):
        prior_ref[k] = carried.astype(jnp.bfloat16)
        factor = pieces_ref[k, rows : rows + 2, :].astype(jnp.float32)
        carried = (factor[0:1] + factor[1:2]) * carried + pieces_ref[k, 0:rows, :].astype(
            jnp.float32
        )


def states_before(sent, axes):
    count, rows, width = sent.shape
    rows = rows - EXTRA
    pieces = lax.all_to_all(sent, axes, 0, 0, tiled=True)
    prior = pl.pallas_call(
        scan_kernel,
        out_shape=jax.ShapeDtypeStruct((count, rows, width), jnp.bfloat16),
        in_specs=[pl.BlockSpec(memory_space=pltpu.VMEM)],
        out_specs=pl.BlockSpec(memory_space=pltpu.VMEM),
        compiler_params=small_vmem(4),
        cost_estimate=pl.CostEstimate(
            flops=3 * count * rows * width, bytes_accessed=4 * count * rows * width, transcendentals=0
        ),
    )(pieces)
    back = lax.all_to_all(prior, axes, 0, 0, tiled=True)
    return back.reshape(count * rows, width)


ALL_AXES = ("section", *CTX, "mp")


def crossed_groups(first):
    sizes = [lax.axis_size(name) for name in ALL_AXES]
    index = np.arange(np.prod(sizes)).reshape(sizes)
    groups = []
    for section in range(sizes[0]):
        for core in range(2):
            grid = index[section, :, :, core]
            groups += (grid if (core == 0) == first else grid.T).tolist()
    return groups


def tail_kernel(wide_ref, narrow_ref, tail_ref):
    width = wide_ref.shape[1]
    tail_ref[:, :width] = wide_ref[...]
    tail_ref[:, width:] = narrow_ref[...]


def last_positions(wide, narrow):
    last = wide.shape[0] // TAIL - 1
    width = wide.shape[1] + narrow.shape[1]
    return pl.pallas_call(
        tail_kernel,
        out_shape=jax.ShapeDtypeStruct((TAIL, width), wide.dtype),
        grid=(1,),
        in_specs=[
            pl.BlockSpec((TAIL, wide.shape[1]), lambda i: (last, 0)),
            pl.BlockSpec((TAIL, narrow.shape[1]), lambda i: (last, 0)),
        ],
        out_specs=pl.BlockSpec((TAIL, width), lambda i: (0, 0)),
        cost_estimate=pl.CostEstimate(flops=0, bytes_accessed=4 * TAIL * width, transcendentals=0),
    )(wide, narrow)


def copies_kernel(rows_ref, copies_ref):
    rows = rows_ref[...]
    for k in range(copies_ref.shape[0]):
        copies_ref[k] = rows


def copied(rows):
    count = lax.axis_size(CTX[0])
    vmem = pl.BlockSpec(memory_space=pltpu.VMEM)
    return pl.pallas_call(
        copies_kernel,
        out_shape=jax.ShapeDtypeStruct((count, *rows.shape), rows.dtype),
        in_specs=[vmem],
        out_specs=vmem,
        compiler_params=small_vmem(4),
        cost_estimate=pl.CostEstimate(
            flops=0, bytes_accessed=2 * (count + 1) * rows.size, transcendentals=0
        ),
    )(rows)


def weight_part(copies):
    pieces = lax.all_to_all(
        copies, ALL_AXES, 0, 0, axis_index_groups=crossed_groups(True), tiled=True
    )
    return pieces.reshape(-1, copies.shape[2])


def prepare_kernel(
    wide_ref,
    narrow_ref,
    behind_ref,
    wide_taps_ref,
    narrow_taps_ref,
    tail_weight_ref,
    factors_ref,
    wide_out_ref,
    narrow_out_ref,
    sent_ref,
    padded_ref,
    weighted_ref,
):
    tokens, width = wide_ref.shape
    heads = tail_weight_ref.shape[0]
    head_width = width // heads
    lanes = 128
    taps = wide_taps_ref.shape[0]
    first = TAIL - taps + 1

    def summed(source_ref, start, behind_start, taps_ref):
        padded_ref[0:TAIL, :] = behind_ref[:, behind_start : behind_start + lanes].astype(
            jnp.float32
        )
        padded_ref[TAIL:, :] = source_ref[:, start : start + lanes].astype(jnp.float32)
        total = jnp.zeros((tokens, lanes), jnp.float32)
        for tap in range(taps):
            total = total + taps_ref[tap : tap + 1, start : start + lanes] * (
                padded_ref[first + tap : first + tap + tokens, :]
            )
        return total

    for start in range(0, narrow_ref.shape[1], lanes):
        narrow_out_ref[:, start : start + lanes] = summed(
            narrow_ref, start, width + start, narrow_taps_ref
        ).astype(jnp.bfloat16)
    for start in range(0, width, lanes):
        active = jax.nn.silu(summed(wide_ref, start, start, wide_taps_ref)).astype(jnp.bfloat16)
        turned = active.astype(jnp.float32).T
        wide_out_ref[start : start + lanes, :] = turned.astype(jnp.bfloat16)
        for part in range(0, lanes, head_width):
            head = (start + part) // head_width
            weighted_ref[start + part : start + part + head_width, :] = (
                turned[part : part + head_width, :] * tail_weight_ref[head : head + 1, :]
            ).astype(jnp.bfloat16)
    state = jnp.dot(
        weighted_ref[...], narrow_out_ref[:, :STATE], preferred_element_type=jnp.float32
    )
    count, _, state_width = sent_ref.shape
    rows = width // count
    sent_ref[:, 0:rows, :] = state.astype(jnp.bfloat16).reshape(count, rows, state_width)
    for k in range(count):
        sent_ref[k, rows:, :] = factors_ref[k * heads // count]


def prepared(wide, narrow, behind, wide_taps, narrow_taps, tail_weight, total_log, axes):
    count = lax.axis_size(axes)
    tokens, width = wide.shape
    high, low = split_in_two(jnp.exp(total_log))
    factors = jnp.stack([high, low] + [jnp.zeros_like(high)] * (EXTRA - 2), axis=1)
    factors = jnp.broadcast_to(factors[:, :, None], (*factors.shape, STATE))
    vmem = pl.BlockSpec(memory_space=pltpu.VMEM)
    return pl.pallas_call(
        prepare_kernel,
        out_shape=(
            jax.ShapeDtypeStruct((width, tokens), jnp.bfloat16),
            jax.ShapeDtypeStruct(narrow.shape, jnp.bfloat16),
            jax.ShapeDtypeStruct((count, width // count + EXTRA, STATE), jnp.bfloat16),
        ),
        in_specs=[vmem] * 7,
        out_specs=(vmem, vmem, vmem),
        scratch_shapes=[
            pltpu.VMEM((TAIL + tokens, 128), jnp.float32),
            pltpu.VMEM((width, tokens), jnp.bfloat16),
        ],
        compiler_params=small_vmem(12),
    cost_estimate=pl.CostEstimate(
        flops=2 * tokens * width * STATE,
        bytes_accessed=8 * tokens * width,
        transcendentals=tokens * width,
    ),
    )(wide, narrow, behind, wide_taps, narrow_taps, tail_weight, factors)


def gathered_weight(part):
    return lax.all_gather(
        part, ALL_AXES, axis_index_groups=crossed_groups(False), axis=0, tiled=True
    )


def assemble_kernel(core_ref, own_ref, other_ref, features_ref, scale_ref, rows_ref):
    half = own_ref.shape[0] - EXTRA
    tokens = own_ref.shape[1]
    ring = CTX_SIDE
    block = half * 2 // (ring * ring)

    @pl.when(core_ref[0] == 0)
    def _():
        rows_ref[0:half, :] = own_ref[0:half, :]
        rows_ref[half : 2 * half, :] = other_ref[0:half, :]

    @pl.when(core_ref[0] != 0)
    def _():
        for outer in range(ring):
            source = other_ref if outer < ring // 2 else own_ref
            for inner in range(ring):
                start = ((outer % (ring // 2)) * ring + inner) * block
                target = (inner * ring + outer) * block
                rows_ref[target : target + block, :] = source[start : start + block, :]

    for start in range(0, 2 * half, tokens):
        part = rows_ref[start : start + tokens, :].astype(jnp.float32)
        features_ref[:, start : start + tokens] = part.T.astype(jnp.bfloat16)
    squares = jnp.sum(
        own_ref[half : half + EXTRA, :].astype(jnp.float32)
        + other_ref[half : half + EXTRA, :].astype(jnp.float32),
        axis=0,
        keepdims=True,
    )
    scale = lax.rsqrt(squares / FEATURES + NORM_FLOOR)
    scale_ref[...] = jnp.broadcast_to(scale, (scale_ref.shape[1], tokens)).T


def assembled(own, other, axis):
    tokens = own.shape[1]
    width = 2 * (own.shape[0] - EXTRA)
    core = lax.axis_index(axis).astype(jnp.int32).reshape(1)
    vmem = pl.BlockSpec(memory_space=pltpu.VMEM)
    return pl.pallas_call(
        assemble_kernel,
        out_shape=(
            jax.ShapeDtypeStruct((tokens, width), jnp.bfloat16),
            jax.ShapeDtypeStruct((tokens, 128), jnp.float32),
        ),
        in_specs=[pl.BlockSpec(memory_space=pltpu.SMEM), vmem, vmem],
        out_specs=(vmem, vmem),
        scratch_shapes=[pltpu.VMEM((width, tokens), jnp.bfloat16)],
        compiler_params=small_vmem(12),
        cost_estimate=pl.CostEstimate(
            flops=4 * tokens * width, bytes_accessed=4 * tokens * width, transcendentals=0
        ),
    )(core, own, other)


def project_kernel(features_ref, scale_ref, weight_ref, out_ref, rows_ref, total_ref, arrived):
    depth, width = rows_ref.shape
    steps = arrived.shape[0]
    block = depth // steps
    part_width = 512

    def fetch(step):
        rows = pl.ds(step * block, block)
        return pltpu.make_async_copy(weight_ref.at[rows], rows_ref.at[rows], arrived.at[step])

    for step in range(steps):
        fetch(step).start()
    for step in range(steps):
        fetch(step).wait()
        for start in range(0, width, part_width):
            columns = slice(start, start + part_width)
            product = jnp.dot(
                features_ref[:, step * block : (step + 1) * block],
                rows_ref[step * block : (step + 1) * block, columns],
                preferred_element_type=jnp.float32,
            )
            if step > 0:
                product = total_ref[:, columns] + product
            if step < steps - 1:
                total_ref[:, columns] = product
            else:
                out_ref[:, columns] = (product * scale_ref[:, 0:1]).astype(out_ref.dtype)


def projected(features, scale, weight, steps=8):
    tokens, depth = features.shape
    width = weight.shape[1]
    vmem = pl.BlockSpec(memory_space=pltpu.VMEM)
    return pl.pallas_call(
        project_kernel,
        out_shape=jax.ShapeDtypeStruct((tokens, width), jnp.bfloat16),
        in_specs=[vmem, vmem, pl.BlockSpec(memory_space=pl.ANY)],
        out_specs=vmem,
        scratch_shapes=[
            pltpu.VMEM((depth, width), weight.dtype),
            pltpu.VMEM((tokens, width), jnp.float32),
            pltpu.SemaphoreType.DMA((steps,)),
        ],
        compiler_params=small_vmem(52),
        cost_estimate=pl.CostEstimate(
            flops=2 * tokens * depth * width, bytes_accessed=2 * depth * width, transcendentals=0
        ),
    )(features, scale, weight)


def other_half(x, axis):
    return lax.ppermute(x, axis, [(0, 1), (1, 0)])


def shifted(value, axis, steps):
    count = lax.axis_size(axis)
    pairs = [(source, (source + steps) % count) for source in range(count)]
    return lax.ppermute(value, axis, pairs)


def section_block(
    head_input,
    state_proj,
    gate_input,
    step_raw,
    step_bias,
    decay_log,
    skip_gain,
    conv_head,
    conv_state,
    norm_gain,
    next_weight,
):
    token_count = head_input.shape[1]
    local_width = head_input.shape[2]
    head_count = step_raw.shape[1]
    head_width = local_width // head_count
    block_count = token_count // BLOCK
    part = weight_part(copied(next_weight[0]))
    tails = last_positions(head_input[0], state_proj[0])
    behind = from_behind(tails, CTX, 1)
    step_size = jax.nn.softplus(step_raw[0] + step_bias[0][:, None])
    log_decay = -jnp.exp(decay_log[0])[:, None] * step_size
    blocks_step = step_size.reshape(head_count, block_count, BLOCK)
    blocks_decay = log_decay.reshape(head_count, block_count, BLOCK)
    row_index = lax.broadcasted_iota(jnp.int32, (BLOCK, BLOCK), 0)
    col_index = lax.broadcasted_iota(jnp.int32, (BLOCK, BLOCK), 1)
    causal_mask = row_index >= col_index
    lower_tri = causal_mask.astype(jnp.float32)
    cumulative = jnp.einsum("hcs,ts->hct", blocks_decay, lower_tri, precision=HIGHEST)
    tail_weight = jnp.exp(cumulative[..., -1:] - cumulative) * blocks_step
    conv_xt, conv_bc, sent = prepared(
        head_input[0],
        state_proj[0],
        behind,
        conv_head[0],
        conv_state[0],
        tail_weight[:, 0],
        cumulative[:, 0, -1],
        CTX,
    )
    blocks_x = conv_xt.T.reshape(block_count, BLOCK, head_count, head_width)
    blocks_b = conv_bc[:, :STATE].reshape(block_count, BLOCK, STATE)
    blocks_c = conv_bc[:, STATE:].reshape(block_count, BLOCK, STATE)
    scores = jnp.einsum("ctn,csn->cts", blocks_c, blocks_b, preferred_element_type=jnp.float32)
    decay_diff = jnp.where(causal_mask, cumulative[..., :, None] - cumulative[..., None, :], 0.0)
    mix_weight = jnp.where(
        causal_mask, scores[None] * jnp.exp(decay_diff) * blocks_step[:, :, None, :], 0.0
    ).astype(jnp.bfloat16)
    intra_part = jnp.einsum(
        "hcts,cshp->cthp", mix_weight, blocks_x, preferred_element_type=jnp.float32
    )
    full_weight = gathered_weight(part)
    prior_state = states_before(sent, CTX).reshape(head_count, head_width, STATE)
    inter_part = (
        jnp.einsum("ctn,hpn->cthp", blocks_c, prior_state, preferred_element_type=jnp.float32)
        * jnp.exp(cumulative).transpose(1, 2, 0)[..., None]
    )
    output = (
        intra_part + inter_part + skip_gain[0][None, None, :, None] * blocks_x.astype(jnp.float32)
    )
    gated = output.reshape(token_count, local_width) * jax.nn.silu(
        gate_input[0].astype(jnp.float32)
    )
    high, low = split_in_two(jnp.sum(gated * gated, axis=1))
    extra = jnp.stack([high, low] + [jnp.zeros_like(high)] * (EXTRA - 2), axis=1)
    features = (gated * norm_gain[0][None]).astype(jnp.bfloat16)
    arrived = shifted(jnp.concatenate([features, extra], axis=1), "section", 1)
    other = other_half(arrived, "mp")
    features, scale = assembled(arrived.T, other.T, "mp")
    return projected(features, scale, full_weight)[None]


def solution(mesh):
    finer = Mesh(
        mesh.devices.reshape(mesh.shape["section"], 8, 8, mesh.shape["mp"]),
        ("section", "ctx_0", "ctx_1", "mp"),
    )
    in_specs = (
        P("section", CTX, "mp"),
        P("section", CTX, None),
        P("section", CTX, "mp"),
        P("section", "mp", CTX),
        P("section", "mp"),
        P("section", "mp"),
        P("section", "mp"),
        P("section", None, "mp"),
        P("section", None, None),
        P("section", "mp"),
        P("section", CTX, "mp"),
    )
    out_specs = P("section", CTX, "mp")
    return jax.shard_map(
        section_block, mesh=finer, in_specs=in_specs, out_specs=out_specs, check_vma=False
    )
```

```python
import jax
import numpy as np
import jax.numpy as jnp
from jax import lax
from jax.experimental import pallas as pl
from jax.experimental.pallas import tpu as pltpu
from jax.sharding import Mesh
from jax.sharding import PartitionSpec as P

STATE = 128
BLOCK = 256
FEATURES = 2048
CTX = ("ctx_0", "ctx_1")
CTX_SIDE = 8
EXTRA = 8
TAIL = 8
WHOLE_VMEM = 67043328


NORM_FLOOR = 0.25


def small_vmem(mebibytes):
    return pltpu.CompilerParams(vmem_limit_bytes=mebibytes * 2**20)


HIGHEST = lax.Precision.HIGHEST


def from_behind(value, axis, steps):
    count = lax.axis_size(axis)
    first, last = (max(0, -steps), min(count, count - steps))
    return lax.ppermute(value, axis, [(source, source + steps) for source in range(first, last)])


def split_in_two(x):
    high = lax.reduce_precision(x, 8, 7)
    return high.astype(jnp.bfloat16), (x - high).astype(jnp.bfloat16)


def scan_kernel(pieces_ref, prior_ref):
    count, _, width = pieces_ref.shape
    rows = prior_ref.shape[1]
    carried = jnp.zeros((rows, width), jnp.float32)
    for k in range(count):
        prior_ref[k] = carried.astype(jnp.bfloat16)
        factor = pieces_ref[k, rows : rows + 2, :].astype(jnp.float32)
        carried = (factor[0:1] + factor[1:2]) * carried + pieces_ref[k, 0:rows, :].astype(
            jnp.float32
        )


def scanned_slices(sent, axes):
    count, rows, width = sent.shape
    rows = rows - EXTRA
    pieces = lax.all_to_all(sent, axes, 0, 0, tiled=True)
    return pl.pallas_call(
        scan_kernel,
        out_shape=jax.ShapeDtypeStruct((count, rows, width), jnp.bfloat16),
        in_specs=[pl.BlockSpec(memory_space=pltpu.VMEM)],
        out_specs=pl.BlockSpec(memory_space=pltpu.VMEM),
        compiler_params=small_vmem(4),
        cost_estimate=pl.CostEstimate(
            flops=3 * count * rows * width, bytes_accessed=4 * count * rows * width, transcendentals=0
        ),
    )(pieces)


ALL_AXES = ("section", *CTX, "mp")


def crossed_groups(first):
    sizes = [lax.axis_size(name) for name in ALL_AXES]
    index = np.arange(np.prod(sizes)).reshape(sizes)
    groups = []
    for section in range(sizes[0]):
        for core in range(2):
            grid = index[section, :, :, core]
            groups += (grid if (core == 0) == first else grid.T).tolist()
    return groups


def tail_kernel(wide_ref, narrow_ref, tail_ref):
    width = wide_ref.shape[1]
    tail_ref[:, :width] = wide_ref[...]
    tail_ref[:, width:] = narrow_ref[...]


def last_positions(wide, narrow):
    last = wide.shape[0] // TAIL - 1
    width = wide.shape[1] + narrow.shape[1]
    return pl.pallas_call(
        tail_kernel,
        out_shape=jax.ShapeDtypeStruct((TAIL, width), wide.dtype),
        grid=(1,),
        in_specs=[
            pl.BlockSpec((TAIL, wide.shape[1]), lambda i: (last, 0)),
            pl.BlockSpec((TAIL, narrow.shape[1]), lambda i: (last, 0)),
        ],
        out_specs=pl.BlockSpec((TAIL, width), lambda i: (0, 0)),
        compiler_params=pltpu.CompilerParams(vmem_limit_bytes=WHOLE_VMEM),
        cost_estimate=pl.CostEstimate(flops=0, bytes_accessed=4 * TAIL * width, transcendentals=0),
    )(wide, narrow)


def copies_kernel(rows_ref, copies_ref, held_ref, loaded, stored):
    count, rows, _ = copies_ref.shape
    chunks = loaded.shape[0]
    size = rows // chunks

    def load(chunk):
        part = pl.ds(chunk * size, size)
        return pltpu.make_async_copy(rows_ref.at[part], held_ref.at[part], loaded.at[chunk])

    def store(chunk, k):
        part = pl.ds(chunk * size, size)
        return pltpu.make_async_copy(
            held_ref.at[part], copies_ref.at[k, part], stored.at[chunk, k]
        )

    for chunk in range(chunks):
        load(chunk).start()
    for chunk in range(chunks):
        load(chunk).wait()
        for k in range(count):
            store(chunk, k).start()
    for chunk in range(chunks):
        for k in range(count):
            store(chunk, k).wait()


def copied(rows, chunks=2):
    count = lax.axis_size(CTX[0])
    anywhere = pl.BlockSpec(memory_space=pl.ANY)
    return pl.pallas_call(
        copies_kernel,
        out_shape=jax.ShapeDtypeStruct((count, *rows.shape), rows.dtype),
        in_specs=[anywhere],
        out_specs=anywhere,
        scratch_shapes=[
            pltpu.VMEM(rows.shape, rows.dtype),
            pltpu.SemaphoreType.DMA((chunks,)),
            pltpu.SemaphoreType.DMA((chunks, count)),
        ],
        cost_estimate=pl.CostEstimate(
            flops=0, bytes_accessed=2 * (count + 1) * rows.size, transcendentals=0
        ),
    )(rows)


def weight_part(copies):
    pieces = lax.all_to_all(
        copies, ALL_AXES, 0, 0, axis_index_groups=crossed_groups(True), tiled=True
    )
    return pieces.reshape(-1, copies.shape[2])


def load_kernel(*refs):
    count = len(refs) // 2
    sems = refs[-1]
    copies = [
        pltpu.make_async_copy(refs[k], refs[count + k], sems.at[k]) for k in range(count)
    ]
    for copy in copies:
        copy.start()
    for copy in copies:
        copy.wait()


def loaded(*arrays):
    vmem = pl.BlockSpec(memory_space=pltpu.VMEM)
    anywhere = pl.BlockSpec(memory_space=pl.ANY)
    return pl.pallas_call(
        load_kernel,
        out_shape=[jax.ShapeDtypeStruct(x.shape, x.dtype) for x in arrays],
        in_specs=[anywhere] * len(arrays),
        out_specs=[vmem] * len(arrays),
        scratch_shapes=[pltpu.SemaphoreType.DMA((len(arrays),))],
        compiler_params=small_vmem(4),
        cost_estimate=pl.CostEstimate(
            flops=0, bytes_accessed=4 * sum(x.size for x in arrays), transcendentals=0
        ),
    )(*arrays)


def prepare_kernel(
    wide_ref,
    narrow_ref,
    behind_ref,
    wide_taps_ref,
    narrow_taps_ref,
    tail_weight_ref,
    factors_ref,
    wide_out_ref,
    narrow_out_ref,
    sent_ref,
    padded_ref,
    weighted_ref,
):
    tokens, width = wide_ref.shape
    heads = tail_weight_ref.shape[0]
    head_width = width // heads
    lanes = 128
    taps = wide_taps_ref.shape[0]
    first = TAIL - taps + 1

    def summed(source_ref, start, behind_start, taps_ref):
        padded_ref[0:TAIL, :] = behind_ref[:, behind_start : behind_start + lanes].astype(
            jnp.float32
        )
        padded_ref[TAIL:, :] = source_ref[:, start : start + lanes].astype(jnp.float32)
        total = jnp.zeros((tokens, lanes), jnp.float32)
        for tap in range(taps):
            total = total + taps_ref[tap : tap + 1, start : start + lanes] * (
                padded_ref[first + tap : first + tap + tokens, :]
            )
        return total

    for start in range(0, narrow_ref.shape[1], lanes):
        narrow_out_ref[:, start : start + lanes] = summed(
            narrow_ref, start, width + start, narrow_taps_ref
        ).astype(jnp.bfloat16)
    for start in range(0, width, lanes):
        active = jax.nn.silu(summed(wide_ref, start, start, wide_taps_ref)).astype(jnp.bfloat16)
        turned = active.astype(jnp.float32).T
        wide_out_ref[start : start + lanes, :] = turned.astype(jnp.bfloat16)
        for part in range(0, lanes, head_width):
            head = (start + part) // head_width
            weighted_ref[start + part : start + part + head_width, :] = (
                turned[part : part + head_width, :] * tail_weight_ref[head : head + 1, :]
            ).astype(jnp.bfloat16)
    state = jnp.dot(
        weighted_ref[...], narrow_out_ref[:, :STATE], preferred_element_type=jnp.float32
    )
    count, _, state_width = sent_ref.shape
    rows = width // count
    sent_ref[:, 0:rows, :] = state.astype(jnp.bfloat16).reshape(count, rows, state_width)
    for k in range(count):
        sent_ref[k, rows:, :] = factors_ref[k * heads // count]


def prepared(wide, narrow, behind, wide_taps, narrow_taps, tail_weight, total_log, axes):
    count = lax.axis_size(axes)
    tokens, width = wide.shape
    high, low = split_in_two(jnp.exp(total_log))
    factors = jnp.stack([high, low] + [jnp.zeros_like(high)] * (EXTRA - 2), axis=1)
    factors = jnp.broadcast_to(factors[:, :, None], (*factors.shape, STATE))
    vmem = pl.BlockSpec(memory_space=pltpu.VMEM)
    return pl.pallas_call(
        prepare_kernel,
        out_shape=(
            jax.ShapeDtypeStruct((width, tokens), jnp.bfloat16),
            jax.ShapeDtypeStruct(narrow.shape, jnp.bfloat16),
            jax.ShapeDtypeStruct((count, width // count + EXTRA, STATE), jnp.bfloat16),
        ),
        in_specs=[vmem] * 7,
        out_specs=(vmem, vmem, vmem),
        scratch_shapes=[
            pltpu.VMEM((TAIL + tokens, 128), jnp.float32),
            pltpu.VMEM((width, tokens), jnp.bfloat16),
        ],
        compiler_params=small_vmem(12),
    cost_estimate=pl.CostEstimate(
        flops=2 * tokens * width * STATE,
        bytes_accessed=8 * tokens * width,
        transcendentals=tokens * width,
    ),
    )(wide, narrow, behind, wide_taps, narrow_taps, tail_weight, factors)


def gathered_weight(part):
    return lax.all_gather(
        part, ALL_AXES, axis_index_groups=crossed_groups(False), axis=0, tiled=True
    )


def assemble_kernel(core_ref, own_ref, other_ref, features_ref, scale_ref, rows_ref):
    half = own_ref.shape[0] - EXTRA
    tokens = own_ref.shape[1]
    ring = CTX_SIDE
    block = half * 2 // (ring * ring)

    @pl.when(core_ref[0] == 0)
    def _():
        rows_ref[0:half, :] = own_ref[0:half, :]
        rows_ref[half : 2 * half, :] = other_ref[0:half, :]

    @pl.when(core_ref[0] != 0)
    def _():
        for outer in range(ring):
            source = other_ref if outer < ring // 2 else own_ref
            for inner in range(ring):
                start = ((outer % (ring // 2)) * ring + inner) * block
                target = (inner * ring + outer) * block
                rows_ref[target : target + block, :] = source[start : start + block, :]

    for start in range(0, 2 * half, tokens):
        part = rows_ref[start : start + tokens, :].astype(jnp.float32)
        features_ref[:, start : start + tokens] = part.T.astype(jnp.bfloat16)
    squares = jnp.sum(
        own_ref[half : half + EXTRA, :].astype(jnp.float32)
        + other_ref[half : half + EXTRA, :].astype(jnp.float32),
        axis=0,
        keepdims=True,
    )
    scale = lax.rsqrt(squares / FEATURES + NORM_FLOOR)
    scale_ref[...] = jnp.broadcast_to(scale, (scale_ref.shape[1], tokens)).T


def assembled(own, other, axis):
    tokens = own.shape[1]
    width = 2 * (own.shape[0] - EXTRA)
    core = lax.axis_index(axis).astype(jnp.int32).reshape(1)
    vmem = pl.BlockSpec(memory_space=pltpu.VMEM)
    return pl.pallas_call(
        assemble_kernel,
        out_shape=(
            jax.ShapeDtypeStruct((tokens, width), jnp.bfloat16),
            jax.ShapeDtypeStruct((tokens, 128), jnp.float32),
        ),
        in_specs=[pl.BlockSpec(memory_space=pltpu.SMEM), vmem, vmem],
        out_specs=(vmem, vmem),
        scratch_shapes=[pltpu.VMEM((width, tokens), jnp.bfloat16)],
        compiler_params=small_vmem(12),
        cost_estimate=pl.CostEstimate(
            flops=4 * tokens * width, bytes_accessed=4 * tokens * width, transcendentals=0
        ),
    )(core, own, other)


def project_kernel(
    features_ref, scale_ref, weight_ref, out_ref, rows_ref, total_ref, arrived, held_ref, left
):
    depth, width = rows_ref.shape
    steps = arrived.shape[0]
    parts = left.shape[0]
    block = depth // steps
    part_width = width // parts

    def fetch(step):
        rows = pl.ds(step * block, block)
        return pltpu.make_async_copy(weight_ref.at[rows], rows_ref.at[rows], arrived.at[step])

    def store(part):
        columns = pl.ds(part * part_width, part_width)
        return pltpu.make_async_copy(held_ref.at[:, columns], out_ref.at[:, columns], left.at[part])

    for step in range(steps):
        fetch(step).start()
    for step in range(steps):
        fetch(step).wait()
        for part in range(parts):
            columns = slice(part * part_width, (part + 1) * part_width)
            product = jnp.dot(
                features_ref[:, step * block : (step + 1) * block],
                rows_ref[step * block : (step + 1) * block, columns],
                preferred_element_type=jnp.float32,
            )
            if step > 0:
                product = total_ref[:, columns] + product
            if step < steps - 1:
                total_ref[:, columns] = product
            else:
                held_ref[:, columns] = (product * scale_ref[:, 0:1]).astype(held_ref.dtype)
                store(part).start()
    for part in range(parts):
        store(part).wait()


def projected(features, scale, weight, steps=8, parts=4):
    tokens, depth = features.shape
    width = weight.shape[1]
    vmem = pl.BlockSpec(memory_space=pltpu.VMEM)
    anywhere = pl.BlockSpec(memory_space=pl.ANY)
    return pl.pallas_call(
        project_kernel,
        out_shape=jax.ShapeDtypeStruct((tokens, width), jnp.bfloat16),
        in_specs=[vmem, vmem, anywhere],
        out_specs=anywhere,
        scratch_shapes=[
            pltpu.VMEM((depth, width), weight.dtype),
            pltpu.VMEM((tokens, width), jnp.float32),
            pltpu.SemaphoreType.DMA((steps,)),
            pltpu.VMEM((tokens, width), jnp.bfloat16),
            pltpu.SemaphoreType.DMA((parts,)),
        ],
        compiler_params=small_vmem(52),
        cost_estimate=pl.CostEstimate(
            flops=2 * tokens * depth * width, bytes_accessed=2 * depth * width, transcendentals=0
        ),
    )(features, scale, weight)


def other_half(x, axis):
    return lax.ppermute(x, axis, [(0, 1), (1, 0)])


def shifted(value, axis, steps):
    count = lax.axis_size(axis)
    pairs = [(source, (source + steps) % count) for source in range(count)]
    return lax.ppermute(value, axis, pairs)


def causal(offset):
    row_index = lax.broadcasted_iota(jnp.int32, (BLOCK, BLOCK), 0)
    col_index = lax.broadcasted_iota(jnp.int32, (BLOCK, BLOCK), 1)
    return row_index >= col_index + offset


def section_block(
    head_input,
    state_proj,
    gate_input,
    step_raw,
    step_bias,
    decay_log,
    skip_gain,
    conv_head,
    conv_state,
    norm_gain,
    next_weight,
):
    token_count = head_input.shape[1]
    local_width = head_input.shape[2]
    head_count = step_raw.shape[1]
    head_width = local_width // head_count
    block_count = token_count // BLOCK
    part = weight_part(copied(next_weight[0]))
    tails = last_positions(head_input[0], state_proj[0])
    behind = from_behind(tails, CTX, 1)
    step_size = jax.nn.softplus(step_raw[0] + step_bias[0][:, None])
    log_decay = -jnp.exp(decay_log[0])[:, None] * step_size
    blocks_step = step_size.reshape(head_count, block_count, BLOCK)
    blocks_decay = log_decay.reshape(head_count, block_count, BLOCK)
    offset = jnp.zeros((), jnp.int32)
    lower_tri = causal(offset).astype(jnp.float32)
    cumulative = jnp.einsum("hcs,ts->hct", blocks_decay, lower_tri, precision=HIGHEST)
    tail_weight = jnp.exp(cumulative[..., -1:] - cumulative) * blocks_step
    wide, narrow, wide_taps, narrow_taps = loaded(
        head_input[0], state_proj[0], conv_head[0], conv_state[0]
    )
    conv_xt, conv_bc, sent = prepared(
        wide,
        narrow,
        behind,
        wide_taps,
        narrow_taps,
        tail_weight[:, 0],
        cumulative[:, 0, -1],
        CTX,
    )
    full_weight = gathered_weight(part)
    prior = scanned_slices(sent, CTX)
    prior, conv_xt, conv_bc, gate_input, offset = lax.optimization_barrier(
        (prior, conv_xt, conv_bc, gate_input, offset)
    )
    prior_state = lax.all_to_all(prior, CTX, 0, 0, tiled=True).reshape(
        head_count, head_width, STATE
    )
    causal_mask = causal(offset)
    blocks_x = conv_xt.T.reshape(block_count, BLOCK, head_count, head_width)
    blocks_b = conv_bc[:, :STATE].reshape(block_count, BLOCK, STATE)
    blocks_c = conv_bc[:, STATE:].reshape(block_count, BLOCK, STATE)
    scores = jnp.einsum("ctn,csn->cts", blocks_c, blocks_b, preferred_element_type=jnp.float32)
    decay_diff = jnp.where(causal_mask, cumulative[..., :, None] - cumulative[..., None, :], 0.0)
    mix_weight = jnp.where(
        causal_mask, scores[None] * jnp.exp(decay_diff) * blocks_step[:, :, None, :], 0.0
    ).astype(jnp.bfloat16)
    intra_part = jnp.einsum(
        "hcts,cshp->cthp", mix_weight, blocks_x, preferred_element_type=jnp.float32
    )
    local_part = intra_part + skip_gain[0][None, None, :, None] * blocks_x.astype(jnp.float32)
    gate = jax.nn.silu(gate_input[0].astype(jnp.float32))
    local_part, gate = lax.optimization_barrier((local_part, gate))
    inter_part = (
        jnp.einsum("ctn,hpn->cthp", blocks_c, prior_state, preferred_element_type=jnp.float32)
        * jnp.exp(cumulative).transpose(1, 2, 0)[..., None]
    )
    gated = (local_part + inter_part).reshape(token_count, local_width) * gate
    high, low = split_in_two(jnp.sum(gated * gated, axis=1))
    extra = jnp.stack([high, low] + [jnp.zeros_like(high)] * (EXTRA - 2), axis=1)
    features = (gated * norm_gain[0][None]).astype(jnp.bfloat16)
    arrived = shifted(jnp.concatenate([features, extra], axis=1), "section", 1)
    other = other_half(arrived, "mp")
    features, scale = assembled(arrived.T, other.T, "mp")
    return projected(features, scale, full_weight)[None]


def solution(mesh):
    finer = Mesh(
        mesh.devices.reshape(mesh.shape["section"], 8, 8, mesh.shape["mp"]),
        ("section", "ctx_0", "ctx_1", "mp"),
    )
    in_specs = (
        P("section", CTX, "mp"),
        P("section", CTX, None),
        P("section", CTX, "mp"),
        P("section", "mp", CTX),
        P("section", "mp"),
        P("section", "mp"),
        P("section", "mp"),
        P("section", None, "mp"),
        P("section", None, None),
        P("section", "mp"),
        P("section", CTX, "mp"),
    )
    out_specs = P("section", CTX, "mp")
    return jax.shard_map(
        section_block, mesh=finer, in_specs=in_specs, out_specs=out_specs, check_vma=False
    )
```

```python
import jax
import numpy as np
import jax.numpy as jnp
from jax import lax
from jax.experimental import pallas as pl
from jax.experimental.pallas import tpu as pltpu
from jax.sharding import Mesh
from jax.sharding import PartitionSpec as P

STATE = 128
BLOCK = 256
FEATURES = 2048
CTX = ("ctx_0", "ctx_1")
CTX_SIDE = 8
EXTRA = 8
PAIR = 2
TAIL = 8
WHOLE_VMEM = 67043328


NORM_FLOOR = 0.25


def small_vmem(mebibytes):
    return pltpu.CompilerParams(vmem_limit_bytes=mebibytes * 2**20)


HIGHEST = lax.Precision.HIGHEST


def from_behind(value, axis, steps):
    count = lax.axis_size(axis)
    first, last = (max(0, -steps), min(count, count - steps))
    return lax.ppermute(value, axis, [(source, source + steps) for source in range(first, last)])


def split_in_two(x):
    high = lax.reduce_precision(x, 8, 7)
    return high.astype(jnp.bfloat16), (x - high).astype(jnp.bfloat16)


def scan_kernel(pieces_ref, prior_ref):
    count, pair, _ = pieces_ref.shape
    _, rows, width = prior_ref.shape
    parts = rows // pair
    carried = [jnp.zeros((pair, width), jnp.float32) for _ in range(parts)]
    for k in range(count):
        factor = pieces_ref[k, :, parts * width :].astype(jnp.float32)
        factor = factor[0:1] + factor[1:2]
        for part in range(parts):
            prior_ref[k, part * pair : (part + 1) * pair, :] = carried[part].astype(jnp.bfloat16)
            piece = pieces_ref[k, :, part * width : (part + 1) * width].astype(jnp.float32)
            carried[part] = factor * carried[part] + piece


def scanned_slices(sent, axes):
    count, pair, total = sent.shape
    width = STATE
    rows = pair * (total // width - 1)
    pieces = lax.all_to_all(sent, axes, 0, 0, tiled=True)
    return pl.pallas_call(
        scan_kernel,
        out_shape=jax.ShapeDtypeStruct((count, rows, width), jnp.bfloat16),
        in_specs=[pl.BlockSpec(memory_space=pltpu.VMEM)],
        out_specs=pl.BlockSpec(memory_space=pltpu.VMEM),
        compiler_params=small_vmem(4),
        cost_estimate=pl.CostEstimate(
            flops=3 * count * rows * width, bytes_accessed=4 * count * rows * width, transcendentals=0
        ),
    )(pieces)


ALL_AXES = ("section", *CTX, "mp")


def crossed_groups(first):
    sizes = [lax.axis_size(name) for name in ALL_AXES]
    index = np.arange(np.prod(sizes)).reshape(sizes)
    groups = []
    for section in range(sizes[0]):
        for core in range(2):
            grid = index[section, :, :, core]
            groups += (grid if (core == 0) == first else grid.T).tolist()
    return groups


def tail_kernel(wide_ref, narrow_ref, tail_ref):
    width = wide_ref.shape[1]
    tail_ref[:, :width] = wide_ref[...]
    tail_ref[:, width:] = narrow_ref[...]


def last_positions(wide, narrow):
    last = wide.shape[0] // TAIL - 1
    width = wide.shape[1] + narrow.shape[1]
    return pl.pallas_call(
        tail_kernel,
        out_shape=jax.ShapeDtypeStruct((TAIL, width), wide.dtype),
        grid=(1,),
        in_specs=[
            pl.BlockSpec((TAIL, wide.shape[1]), lambda i: (last, 0)),
            pl.BlockSpec((TAIL, narrow.shape[1]), lambda i: (last, 0)),
        ],
        out_specs=pl.BlockSpec((TAIL, width), lambda i: (0, 0)),
        compiler_params=pltpu.CompilerParams(vmem_limit_bytes=WHOLE_VMEM),
        cost_estimate=pl.CostEstimate(flops=0, bytes_accessed=4 * TAIL * width, transcendentals=0),
    )(wide, narrow)


def copies_kernel(rows_ref, copies_ref, held_ref, loaded, stored):
    count, rows, _ = copies_ref.shape
    chunks = loaded.shape[0]
    size = rows // chunks

    def load(chunk):
        part = pl.ds(chunk * size, size)
        return pltpu.make_async_copy(rows_ref.at[part], held_ref.at[part], loaded.at[chunk])

    def store(chunk, k):
        part = pl.ds(chunk * size, size)
        return pltpu.make_async_copy(
            held_ref.at[part], copies_ref.at[k, part], stored.at[chunk, k]
        )

    for chunk in range(chunks):
        load(chunk).start()
    for chunk in range(chunks):
        load(chunk).wait()
        for k in range(count):
            store(chunk, k).start()
    for chunk in range(chunks):
        for k in range(count):
            store(chunk, k).wait()


def copied(rows, chunks=2):
    count = lax.axis_size(CTX[0])
    anywhere = pl.BlockSpec(memory_space=pl.ANY)
    return pl.pallas_call(
        copies_kernel,
        out_shape=jax.ShapeDtypeStruct((count, *rows.shape), rows.dtype),
        in_specs=[anywhere],
        out_specs=anywhere,
        scratch_shapes=[
            pltpu.VMEM(rows.shape, rows.dtype),
            pltpu.SemaphoreType.DMA((chunks,)),
            pltpu.SemaphoreType.DMA((chunks, count)),
        ],
        cost_estimate=pl.CostEstimate(
            flops=0, bytes_accessed=2 * (count + 1) * rows.size, transcendentals=0
        ),
    )(rows)


def weight_part(copies):
    pieces = lax.all_to_all(
        copies, ALL_AXES, 0, 0, axis_index_groups=crossed_groups(True), tiled=True
    )
    return pieces.reshape(-1, copies.shape[2])


def load_kernel(*refs):
    count = len(refs) // 2
    sems = refs[-1]
    copies = [
        pltpu.make_async_copy(refs[k], refs[count + k], sems.at[k]) for k in range(count)
    ]
    for copy in copies:
        copy.start()
    for copy in copies:
        copy.wait()


def loaded(*arrays):
    vmem = pl.BlockSpec(memory_space=pltpu.VMEM)
    anywhere = pl.BlockSpec(memory_space=pl.ANY)
    return pl.pallas_call(
        load_kernel,
        out_shape=[jax.ShapeDtypeStruct(x.shape, x.dtype) for x in arrays],
        in_specs=[anywhere] * len(arrays),
        out_specs=[vmem] * len(arrays),
        scratch_shapes=[pltpu.SemaphoreType.DMA((len(arrays),))],
        compiler_params=small_vmem(4),
        cost_estimate=pl.CostEstimate(
            flops=0, bytes_accessed=4 * sum(x.size for x in arrays), transcendentals=0
        ),
    )(*arrays)


def prepare_kernel(
    wide_ref,
    narrow_ref,
    behind_ref,
    wide_taps_ref,
    narrow_taps_ref,
    tail_weight_ref,
    factors_ref,
    wide_out_ref,
    narrow_out_ref,
    sent_ref,
    padded_ref,
    weighted_ref,
    state_ref,
):
    tokens, width = wide_ref.shape
    heads = tail_weight_ref.shape[0]
    head_width = width // heads
    lanes = 128
    taps = wide_taps_ref.shape[0]
    first = TAIL - taps + 1

    def summed(source_ref, start, behind_start, taps_ref):
        padded_ref[0:TAIL, :] = behind_ref[:, behind_start : behind_start + lanes].astype(
            jnp.float32
        )
        padded_ref[TAIL:, :] = source_ref[:, start : start + lanes].astype(jnp.float32)
        total = jnp.zeros((tokens, lanes), jnp.float32)
        for tap in range(taps):
            total = total + taps_ref[tap : tap + 1, start : start + lanes] * (
                padded_ref[first + tap : first + tap + tokens, :]
            )
        return total

    for start in range(0, narrow_ref.shape[1], lanes):
        narrow_out_ref[:, start : start + lanes] = summed(
            narrow_ref, start, width + start, narrow_taps_ref
        ).astype(jnp.bfloat16)
    for start in range(0, width, lanes):
        active = jax.nn.silu(summed(wide_ref, start, start, wide_taps_ref)).astype(jnp.bfloat16)
        turned = active.astype(jnp.float32).T
        wide_out_ref[start : start + lanes, :] = turned.astype(jnp.bfloat16)
        for part in range(0, lanes, head_width):
            head = (start + part) // head_width
            weighted_ref[start + part : start + part + head_width, :] = (
                turned[part : part + head_width, :] * tail_weight_ref[head : head + 1, :]
            ).astype(jnp.bfloat16)
    state = jnp.dot(
        weighted_ref[...], narrow_out_ref[:, :STATE], preferred_element_type=jnp.float32
    )
    state_ref[...] = state
    count, pair, total = sent_ref.shape
    parts = total // STATE - 1
    for k in range(count):
        for part in range(parts):
            start = (k * parts + part) * pair
            sent_ref[k, :, part * STATE : (part + 1) * STATE] = state_ref[
                start : start + pair, :
            ].astype(jnp.bfloat16)
        sent_ref[k, :, parts * STATE :] = factors_ref[k * heads // count, 0:pair, :]


def prepared(wide, narrow, behind, wide_taps, narrow_taps, tail_weight, total_log, axes):
    count = lax.axis_size(axes)
    tokens, width = wide.shape
    high, low = split_in_two(jnp.exp(total_log))
    factors = jnp.stack([high, low] + [jnp.zeros_like(high)] * (EXTRA - 2), axis=1)
    factors = jnp.broadcast_to(factors[:, :, None], (*factors.shape, STATE))
    slice_width = (width // count // PAIR + 1) * STATE
    vmem = pl.BlockSpec(memory_space=pltpu.VMEM)
    return pl.pallas_call(
        prepare_kernel,
        out_shape=(
            jax.ShapeDtypeStruct((width, tokens), jnp.bfloat16),
            jax.ShapeDtypeStruct(narrow.shape, jnp.bfloat16),
            jax.ShapeDtypeStruct((count, PAIR, slice_width), jnp.bfloat16),
        ),
        in_specs=[vmem] * 7,
        out_specs=(vmem, vmem, vmem),
        scratch_shapes=[
            pltpu.VMEM((TAIL + tokens, 128), jnp.float32),
            pltpu.VMEM((width, tokens), jnp.bfloat16),
            pltpu.VMEM((width, STATE), jnp.float32),
        ],
        compiler_params=small_vmem(12),
    cost_estimate=pl.CostEstimate(
        flops=2 * tokens * width * STATE,
        bytes_accessed=8 * tokens * width,
        transcendentals=tokens * width,
    ),
    )(wide, narrow, behind, wide_taps, narrow_taps, tail_weight, factors)


def gathered_weight(part):
    return lax.all_gather(
        part, ALL_AXES, axis_index_groups=crossed_groups(False), axis=0, tiled=True
    )


def assemble_kernel(core_ref, own_ref, other_ref, features_ref, scale_ref, rows_ref):
    half = own_ref.shape[0] - EXTRA
    tokens = own_ref.shape[1]
    ring = CTX_SIDE
    block = half * 2 // (ring * ring)

    @pl.when(core_ref[0] == 0)
    def _():
        rows_ref[0:half, :] = own_ref[0:half, :]
        rows_ref[half : 2 * half, :] = other_ref[0:half, :]

    @pl.when(core_ref[0] != 0)
    def _():
        for outer in range(ring):
            source = other_ref if outer < ring // 2 else own_ref
            for inner in range(ring):
                start = ((outer % (ring // 2)) * ring + inner) * block
                target = (inner * ring + outer) * block
                rows_ref[target : target + block, :] = source[start : start + block, :]

    for start in range(0, 2 * half, tokens):
        part = rows_ref[start : start + tokens, :].astype(jnp.float32)
        features_ref[:, start : start + tokens] = part.T.astype(jnp.bfloat16)
    squares = jnp.sum(
        own_ref[half : half + EXTRA, :].astype(jnp.float32)
        + other_ref[half : half + EXTRA, :].astype(jnp.float32),
        axis=0,
        keepdims=True,
    )
    scale = lax.rsqrt(squares / FEATURES + NORM_FLOOR)
    scale_ref[...] = jnp.broadcast_to(scale, (scale_ref.shape[1], tokens)).T


def assembled(own, other, axis):
    tokens = own.shape[1]
    width = 2 * (own.shape[0] - EXTRA)
    core = lax.axis_index(axis).astype(jnp.int32).reshape(1)
    vmem = pl.BlockSpec(memory_space=pltpu.VMEM)
    return pl.pallas_call(
        assemble_kernel,
        out_shape=(
            jax.ShapeDtypeStruct((tokens, width), jnp.bfloat16),
            jax.ShapeDtypeStruct((tokens, 128), jnp.float32),
        ),
        in_specs=[pl.BlockSpec(memory_space=pltpu.SMEM), vmem, vmem],
        out_specs=(vmem, vmem),
        scratch_shapes=[pltpu.VMEM((width, tokens), jnp.bfloat16)],
        compiler_params=small_vmem(12),
        cost_estimate=pl.CostEstimate(
            flops=4 * tokens * width, bytes_accessed=4 * tokens * width, transcendentals=0
        ),
    )(core, own, other)


def project_kernel(
    features_ref, scale_ref, weight_ref, out_ref, rows_ref, total_ref, arrived, held_ref, left
):
    depth, width = rows_ref.shape
    steps = arrived.shape[0]
    parts = left.shape[0]
    block = depth // steps
    part_width = width // parts

    def fetch(step):
        rows = pl.ds(step * block, block)
        return pltpu.make_async_copy(weight_ref.at[rows], rows_ref.at[rows], arrived.at[step])

    def store(part):
        columns = pl.ds(part * part_width, part_width)
        return pltpu.make_async_copy(held_ref.at[:, columns], out_ref.at[:, columns], left.at[part])

    for step in range(steps):
        fetch(step).start()
    for step in range(steps):
        fetch(step).wait()
        for part in range(parts):
            columns = slice(part * part_width, (part + 1) * part_width)
            product = jnp.dot(
                features_ref[:, step * block : (step + 1) * block],
                rows_ref[step * block : (step + 1) * block, columns],
                preferred_element_type=jnp.float32,
            )
            if step > 0:
                product = total_ref[:, columns] + product
            if step < steps - 1:
                total_ref[:, columns] = product
            else:
                held_ref[:, columns] = (product * scale_ref[:, 0:1]).astype(held_ref.dtype)
                store(part).start()
    for part in range(parts):
        store(part).wait()


def projected(features, scale, weight, steps=8, parts=4):
    tokens, depth = features.shape
    width = weight.shape[1]
    vmem = pl.BlockSpec(memory_space=pltpu.VMEM)
    anywhere = pl.BlockSpec(memory_space=pl.ANY)
    return pl.pallas_call(
        project_kernel,
        out_shape=jax.ShapeDtypeStruct((tokens, width), jnp.bfloat16),
        in_specs=[vmem, vmem, anywhere],
        out_specs=anywhere,
        scratch_shapes=[
            pltpu.VMEM((depth, width), weight.dtype),
            pltpu.VMEM((tokens, width), jnp.float32),
            pltpu.SemaphoreType.DMA((steps,)),
            pltpu.VMEM((tokens, width), jnp.bfloat16),
            pltpu.SemaphoreType.DMA((parts,)),
        ],
        compiler_params=small_vmem(52),
        cost_estimate=pl.CostEstimate(
            flops=2 * tokens * depth * width, bytes_accessed=2 * depth * width, transcendentals=0
        ),
    )(features, scale, weight)


def other_half(x, axis):
    return lax.ppermute(x, axis, [(0, 1), (1, 0)])


def shifted(value, axis, steps):
    count = lax.axis_size(axis)
    pairs = [(source, (source + steps) % count) for source in range(count)]
    return lax.ppermute(value, axis, pairs)


def causal(offset):
    row_index = lax.broadcasted_iota(jnp.int32, (BLOCK, BLOCK), 0)
    col_index = lax.broadcasted_iota(jnp.int32, (BLOCK, BLOCK), 1)
    return row_index >= col_index + offset


def section_block(
    head_input,
    state_proj,
    gate_input,
    step_raw,
    step_bias,
    decay_log,
    skip_gain,
    conv_head,
    conv_state,
    norm_gain,
    next_weight,
):
    token_count = head_input.shape[1]
    local_width = head_input.shape[2]
    head_count = step_raw.shape[1]
    head_width = local_width // head_count
    block_count = token_count // BLOCK
    part = weight_part(copied(next_weight[0]))
    tails = last_positions(head_input[0], state_proj[0])
    behind = from_behind(tails, CTX, 1)
    step_size = jax.nn.softplus(step_raw[0] + step_bias[0][:, None])
    log_decay = -jnp.exp(decay_log[0])[:, None] * step_size
    blocks_step = step_size.reshape(head_count, block_count, BLOCK)
    blocks_decay = log_decay.reshape(head_count, block_count, BLOCK)
    offset = jnp.zeros((), jnp.int32)
    lower_tri = causal(offset).astype(jnp.float32)
    cumulative = jnp.einsum("hcs,ts->hct", blocks_decay, lower_tri, precision=HIGHEST)
    tail_weight = jnp.exp(cumulative[..., -1:] - cumulative) * blocks_step
    wide, narrow, wide_taps, narrow_taps = loaded(
        head_input[0], state_proj[0], conv_head[0], conv_state[0]
    )
    conv_xt, conv_bc, sent = prepared(
        wide,
        narrow,
        behind,
        wide_taps,
        narrow_taps,
        tail_weight[:, 0],
        cumulative[:, 0, -1],
        CTX,
    )
    full_weight = gathered_weight(part)
    prior = scanned_slices(sent, CTX)
    prior, conv_xt, conv_bc, gate_input, offset = lax.optimization_barrier(
        (prior, conv_xt, conv_bc, gate_input, offset)
    )
    prior_state = lax.all_to_all(prior, CTX, 0, 0, tiled=True).reshape(
        head_count, head_width, STATE
    )
    causal_mask = causal(offset)
    blocks_x = conv_xt.T.reshape(block_count, BLOCK, head_count, head_width)
    blocks_b = conv_bc[:, :STATE].reshape(block_count, BLOCK, STATE)
    blocks_c = conv_bc[:, STATE:].reshape(block_count, BLOCK, STATE)
    scores = jnp.einsum("ctn,csn->cts", blocks_c, blocks_b, preferred_element_type=jnp.float32)
    decay_diff = jnp.where(causal_mask, cumulative[..., :, None] - cumulative[..., None, :], 0.0)
    mix_weight = jnp.where(
        causal_mask, scores[None] * jnp.exp(decay_diff) * blocks_step[:, :, None, :], 0.0
    ).astype(jnp.bfloat16)
    intra_part = jnp.einsum(
        "hcts,cshp->cthp", mix_weight, blocks_x, preferred_element_type=jnp.float32
    )
    local_part = intra_part + skip_gain[0][None, None, :, None] * blocks_x.astype(jnp.float32)
    gate = jax.nn.silu(gate_input[0].astype(jnp.float32))
    local_part, gate = lax.optimization_barrier((local_part, gate))
    inter_part = (
        jnp.einsum("ctn,hpn->cthp", blocks_c, prior_state, preferred_element_type=jnp.float32)
        * jnp.exp(cumulative).transpose(1, 2, 0)[..., None]
    )
    gated = (local_part + inter_part).reshape(token_count, local_width) * gate
    high, low = split_in_two(jnp.sum(gated * gated, axis=1))
    extra = jnp.stack([high, low] + [jnp.zeros_like(high)] * (EXTRA - 2), axis=1)
    features = (gated * norm_gain[0][None]).astype(jnp.bfloat16)
    arrived = shifted(jnp.concatenate([features, extra], axis=1), "section", 1)
    other = other_half(arrived, "mp")
    features, scale = assembled(arrived.T, other.T, "mp")
    return projected(features, scale, full_weight)[None]


def solution(mesh):
    finer = Mesh(
        mesh.devices.reshape(mesh.shape["section"], 8, 8, mesh.shape["mp"]),
        ("section", "ctx_0", "ctx_1", "mp"),
    )
    in_specs = (
        P("section", CTX, "mp"),
        P("section", CTX, None),
        P("section", CTX, "mp"),
        P("section", "mp", CTX),
        P("section", "mp"),
        P("section", "mp"),
        P("section", "mp"),
        P("section", None, "mp"),
        P("section", None, None),
        P("section", "mp"),
        P("section", CTX, "mp"),
    )
    out_specs = P("section", CTX, "mp")
    return jax.shard_map(
        section_block, mesh=finer, in_specs=in_specs, out_specs=out_specs, check_vma=False
    )
```

```python
import jax
import numpy as np
import jax.numpy as jnp
from jax import lax
from jax.experimental import pallas as pl
from jax.experimental.pallas import tpu as pltpu
from jax.sharding import Mesh
from jax.sharding import PartitionSpec as P

STATE = 128
BLOCK = 256
FEATURES = 2048
CTX = ("ctx_0", "ctx_1")
CTX_SIDE = 8
EXTRA = 8
PAIR = 2
TAIL = 8
WHOLE_VMEM = 67043328


NORM_FLOOR = 0.25


def small_vmem(mebibytes):
    return pltpu.CompilerParams(vmem_limit_bytes=mebibytes * 2**20)


HIGHEST = lax.Precision.HIGHEST


def from_behind(value, axis, steps):
    count = lax.axis_size(axis)
    first, last = (max(0, -steps), min(count, count - steps))
    return lax.ppermute(value, axis, [(source, source + steps) for source in range(first, last)])


def split_in_two(x):
    high = lax.reduce_precision(x, 8, 7)
    return high.astype(jnp.bfloat16), (x - high).astype(jnp.bfloat16)


def scan_kernel(pieces_ref, prior_ref):
    count, pair, _ = pieces_ref.shape
    _, rows, width = prior_ref.shape
    parts = rows // pair
    carried = [jnp.zeros((pair, width), jnp.float32) for _ in range(parts)]
    for k in range(count):
        factor = pieces_ref[k, :, parts * width :].astype(jnp.float32)
        factor = factor[0:1] + factor[1:2]
        for part in range(parts):
            prior_ref[k, part * pair : (part + 1) * pair, :] = carried[part].astype(jnp.bfloat16)
            piece = pieces_ref[k, :, part * width : (part + 1) * width].astype(jnp.float32)
            carried[part] = factor * carried[part] + piece


def scanned_slices(sent, axes):
    count, pair, total = sent.shape
    width = STATE
    rows = pair * (total // width - 1)
    pieces = lax.all_to_all(sent, axes, 0, 0, tiled=True)
    return pl.pallas_call(
        scan_kernel,
        out_shape=jax.ShapeDtypeStruct((count, rows, width), jnp.bfloat16),
        in_specs=[pl.BlockSpec(memory_space=pltpu.VMEM)],
        out_specs=pl.BlockSpec(memory_space=pltpu.VMEM),
        compiler_params=small_vmem(4),
        cost_estimate=pl.CostEstimate(
            flops=3 * count * rows * width, bytes_accessed=4 * count * rows * width, transcendentals=0
        ),
    )(pieces)


ALL_AXES = ("section", *CTX, "mp")


def crossed_groups(first):
    sizes = [lax.axis_size(name) for name in ALL_AXES]
    index = np.arange(np.prod(sizes)).reshape(sizes)
    groups = []
    for section in range(sizes[0]):
        for core in range(2):
            grid = index[section, :, :, core]
            groups += (grid if (core == 1) == first else grid.T).tolist()
    return groups


def tail_kernel(wide_ref, narrow_ref, tail_ref):
    width = wide_ref.shape[1]
    tail_ref[:, :width] = wide_ref[...]
    tail_ref[:, width:] = narrow_ref[...]


def last_positions(wide, narrow):
    last = wide.shape[0] // TAIL - 1
    width = wide.shape[1] + narrow.shape[1]
    return pl.pallas_call(
        tail_kernel,
        out_shape=jax.ShapeDtypeStruct((TAIL, width), wide.dtype),
        grid=(1,),
        in_specs=[
            pl.BlockSpec((TAIL, wide.shape[1]), lambda i: (last, 0)),
            pl.BlockSpec((TAIL, narrow.shape[1]), lambda i: (last, 0)),
        ],
        out_specs=pl.BlockSpec((TAIL, width), lambda i: (0, 0)),
        compiler_params=pltpu.CompilerParams(vmem_limit_bytes=WHOLE_VMEM),
        cost_estimate=pl.CostEstimate(flops=0, bytes_accessed=4 * TAIL * width, transcendentals=0),
    )(wide, narrow)


def copies_kernel(rows_ref, copies_ref, held_ref, loaded, stored):
    count, rows, _ = copies_ref.shape
    chunks = loaded.shape[0]
    size = rows // chunks

    def load(chunk):
        part = pl.ds(chunk * size, size)
        return pltpu.make_async_copy(rows_ref.at[part], held_ref.at[part], loaded.at[chunk])

    def store(chunk, k):
        part = pl.ds(chunk * size, size)
        return pltpu.make_async_copy(
            held_ref.at[part], copies_ref.at[k, part], stored.at[chunk, k]
        )

    for chunk in range(chunks):
        load(chunk).start()
    for chunk in range(chunks):
        load(chunk).wait()
        for k in range(count):
            store(chunk, k).start()
    for chunk in range(chunks):
        for k in range(count):
            store(chunk, k).wait()


def copied(rows, chunks=2):
    count = lax.axis_size(CTX[0])
    anywhere = pl.BlockSpec(memory_space=pl.ANY)
    return pl.pallas_call(
        copies_kernel,
        out_shape=jax.ShapeDtypeStruct((count, *rows.shape), rows.dtype),
        in_specs=[anywhere],
        out_specs=anywhere,
        scratch_shapes=[
            pltpu.VMEM(rows.shape, rows.dtype),
            pltpu.SemaphoreType.DMA((chunks,)),
            pltpu.SemaphoreType.DMA((chunks, count)),
        ],
        cost_estimate=pl.CostEstimate(
            flops=0, bytes_accessed=2 * (count + 1) * rows.size, transcendentals=0
        ),
    )(rows)


def weight_part(copies):
    pieces = lax.all_to_all(
        copies, ALL_AXES, 0, 0, axis_index_groups=crossed_groups(True), tiled=True
    )
    return pieces.reshape(-1, copies.shape[2])


def load_kernel(*refs):
    count = len(refs) // 2
    sems = refs[-1]
    copies = [
        pltpu.make_async_copy(refs[k], refs[count + k], sems.at[k]) for k in range(count)
    ]
    for copy in copies:
        copy.start()
    for copy in copies:
        copy.wait()


def loaded(*arrays):
    vmem = pl.BlockSpec(memory_space=pltpu.VMEM)
    anywhere = pl.BlockSpec(memory_space=pl.ANY)
    return pl.pallas_call(
        load_kernel,
        out_shape=[jax.ShapeDtypeStruct(x.shape, x.dtype) for x in arrays],
        in_specs=[anywhere] * len(arrays),
        out_specs=[vmem] * len(arrays),
        scratch_shapes=[pltpu.SemaphoreType.DMA((len(arrays),))],
        compiler_params=small_vmem(4),
        cost_estimate=pl.CostEstimate(
            flops=0, bytes_accessed=4 * sum(x.size for x in arrays), transcendentals=0
        ),
    )(*arrays)


def prepare_kernel(
    wide_ref,
    narrow_ref,
    behind_ref,
    wide_taps_ref,
    narrow_taps_ref,
    tail_weight_ref,
    factors_ref,
    wide_out_ref,
    narrow_out_ref,
    sent_ref,
    padded_ref,
    weighted_ref,
    state_ref,
):
    tokens, width = wide_ref.shape
    heads = tail_weight_ref.shape[0]
    head_width = width // heads
    lanes = 128
    taps = wide_taps_ref.shape[0]
    first = TAIL - taps + 1

    def summed(source_ref, start, behind_start, taps_ref):
        padded_ref[0:TAIL, :] = behind_ref[:, behind_start : behind_start + lanes].astype(
            jnp.float32
        )
        padded_ref[TAIL:, :] = source_ref[:, start : start + lanes].astype(jnp.float32)
        total = jnp.zeros((tokens, lanes), jnp.float32)
        for tap in range(taps):
            total = total + taps_ref[tap : tap + 1, start : start + lanes] * (
                padded_ref[first + tap : first + tap + tokens, :]
            )
        return total

    for start in range(0, narrow_ref.shape[1], lanes):
        narrow_out_ref[:, start : start + lanes] = summed(
            narrow_ref, start, width + start, narrow_taps_ref
        ).astype(jnp.bfloat16)
    for start in range(0, width, lanes):
        active = jax.nn.silu(summed(wide_ref, start, start, wide_taps_ref)).astype(jnp.bfloat16)
        turned = active.astype(jnp.float32).T
        wide_out_ref[start : start + lanes, :] = turned.astype(jnp.bfloat16)
        for part in range(0, lanes, head_width):
            head = (start + part) // head_width
            weighted_ref[start + part : start + part + head_width, :] = (
                turned[part : part + head_width, :] * tail_weight_ref[head : head + 1, :]
            ).astype(jnp.bfloat16)
    state = jnp.dot(
        weighted_ref[...], narrow_out_ref[:, :STATE], preferred_element_type=jnp.float32
    )
    state_ref[...] = state
    count, pair, total = sent_ref.shape
    parts = total // STATE - 1
    for k in range(count):
        for part in range(parts):
            start = (k * parts + part) * pair
            sent_ref[k, :, part * STATE : (part + 1) * STATE] = state_ref[
                start : start + pair, :
            ].astype(jnp.bfloat16)
        sent_ref[k, :, parts * STATE :] = factors_ref[k * heads // count, 0:pair, :]


def prepared(wide, narrow, behind, wide_taps, narrow_taps, tail_weight, total_log, axes):
    count = lax.axis_size(axes)
    tokens, width = wide.shape
    high, low = split_in_two(jnp.exp(total_log))
    factors = jnp.stack([high, low] + [jnp.zeros_like(high)] * (EXTRA - 2), axis=1)
    factors = jnp.broadcast_to(factors[:, :, None], (*factors.shape, STATE))
    slice_width = (width // count // PAIR + 1) * STATE
    vmem = pl.BlockSpec(memory_space=pltpu.VMEM)
    return pl.pallas_call(
        prepare_kernel,
        out_shape=(
            jax.ShapeDtypeStruct((width, tokens), jnp.bfloat16),
            jax.ShapeDtypeStruct(narrow.shape, jnp.bfloat16),
            jax.ShapeDtypeStruct((count, PAIR, slice_width), jnp.bfloat16),
        ),
        in_specs=[vmem] * 7,
        out_specs=(vmem, vmem, vmem),
        scratch_shapes=[
            pltpu.VMEM((TAIL + tokens, 128), jnp.float32),
            pltpu.VMEM((width, tokens), jnp.bfloat16),
            pltpu.VMEM((width, STATE), jnp.float32),
        ],
        compiler_params=small_vmem(12),
    cost_estimate=pl.CostEstimate(
        flops=2 * tokens * width * STATE,
        bytes_accessed=8 * tokens * width,
        transcendentals=tokens * width,
    ),
    )(wide, narrow, behind, wide_taps, narrow_taps, tail_weight, factors)


def gathered_weight(part):
    return lax.all_gather(
        part, ALL_AXES, axis_index_groups=crossed_groups(False), axis=0, tiled=True
    )


def assemble_kernel(core_ref, own_ref, other_ref, features_ref, scale_ref, rows_ref):
    half = own_ref.shape[0] - EXTRA
    tokens = own_ref.shape[1]
    ring = CTX_SIDE
    block = half * 2 // (ring * ring)

    @pl.when(core_ref[0] != 0)
    def _():
        rows_ref[0:half, :] = other_ref[0:half, :]
        rows_ref[half : 2 * half, :] = own_ref[0:half, :]

    @pl.when(core_ref[0] == 0)
    def _():
        for outer in range(ring):
            source = own_ref if outer < ring // 2 else other_ref
            for inner in range(ring):
                start = ((outer % (ring // 2)) * ring + inner) * block
                target = (inner * ring + outer) * block
                rows_ref[target : target + block, :] = source[start : start + block, :]

    for start in range(0, 2 * half, tokens):
        part = rows_ref[start : start + tokens, :].astype(jnp.float32)
        features_ref[:, start : start + tokens] = part.T.astype(jnp.bfloat16)
    squares = jnp.sum(
        own_ref[half : half + EXTRA, :].astype(jnp.float32)
        + other_ref[half : half + EXTRA, :].astype(jnp.float32),
        axis=0,
        keepdims=True,
    )
    scale = lax.rsqrt(squares / FEATURES + NORM_FLOOR)
    scale_ref[...] = jnp.broadcast_to(scale, (scale_ref.shape[1], tokens)).T


def assembled(own, other, axis):
    tokens = own.shape[1]
    width = 2 * (own.shape[0] - EXTRA)
    core = lax.axis_index(axis).astype(jnp.int32).reshape(1)
    vmem = pl.BlockSpec(memory_space=pltpu.VMEM)
    return pl.pallas_call(
        assemble_kernel,
        out_shape=(
            jax.ShapeDtypeStruct((tokens, width), jnp.bfloat16),
            jax.ShapeDtypeStruct((tokens, 128), jnp.float32),
        ),
        in_specs=[pl.BlockSpec(memory_space=pltpu.SMEM), vmem, vmem],
        out_specs=(vmem, vmem),
        scratch_shapes=[pltpu.VMEM((width, tokens), jnp.bfloat16)],
        compiler_params=small_vmem(12),
        cost_estimate=pl.CostEstimate(
            flops=4 * tokens * width, bytes_accessed=4 * tokens * width, transcendentals=0
        ),
    )(core, own, other)


def project_kernel(
    features_ref, scale_ref, weight_ref, out_ref, rows_ref, total_ref, arrived, held_ref, left
):
    depth, width = rows_ref.shape
    steps = arrived.shape[0]
    parts = left.shape[0]
    block = depth // steps
    part_width = width // parts

    def fetch(step):
        rows = pl.ds(step * block, block)
        return pltpu.make_async_copy(weight_ref.at[rows], rows_ref.at[rows], arrived.at[step])

    def store(part):
        columns = pl.ds(part * part_width, part_width)
        return pltpu.make_async_copy(held_ref.at[:, columns], out_ref.at[:, columns], left.at[part])

    for step in range(steps):
        fetch(step).start()
    for step in range(steps):
        fetch(step).wait()
        for part in range(parts):
            columns = slice(part * part_width, (part + 1) * part_width)
            product = jnp.dot(
                features_ref[:, step * block : (step + 1) * block],
                rows_ref[step * block : (step + 1) * block, columns],
                preferred_element_type=jnp.float32,
            )
            if step > 0:
                product = total_ref[:, columns] + product
            if step < steps - 1:
                total_ref[:, columns] = product
            else:
                held_ref[:, columns] = (product * scale_ref[:, 0:1]).astype(held_ref.dtype)
                store(part).start()
    for part in range(parts):
        store(part).wait()


def projected(features, scale, weight, steps=8, parts=4):
    tokens, depth = features.shape
    width = weight.shape[1]
    vmem = pl.BlockSpec(memory_space=pltpu.VMEM)
    anywhere = pl.BlockSpec(memory_space=pl.ANY)
    return pl.pallas_call(
        project_kernel,
        out_shape=jax.ShapeDtypeStruct((tokens, width), jnp.bfloat16),
        in_specs=[vmem, vmem, anywhere],
        out_specs=anywhere,
        scratch_shapes=[
            pltpu.VMEM((depth, width), weight.dtype),
            pltpu.VMEM((tokens, width), jnp.float32),
            pltpu.SemaphoreType.DMA((steps,)),
            pltpu.VMEM((tokens, width), jnp.bfloat16),
            pltpu.SemaphoreType.DMA((parts,)),
        ],
        compiler_params=small_vmem(52),
        cost_estimate=pl.CostEstimate(
            flops=2 * tokens * depth * width, bytes_accessed=2 * depth * width, transcendentals=0
        ),
    )(features, scale, weight)


def other_half(x, axis):
    return lax.ppermute(x, axis, [(0, 1), (1, 0)])


def shifted(value, axis, steps):
    count = lax.axis_size(axis)
    pairs = [(source, (source + steps) % count) for source in range(count)]
    return lax.ppermute(value, axis, pairs)


def causal(offset):
    row_index = lax.broadcasted_iota(jnp.int32, (BLOCK, BLOCK), 0)
    col_index = lax.broadcasted_iota(jnp.int32, (BLOCK, BLOCK), 1)
    return row_index >= col_index + offset


def section_block(
    head_input,
    state_proj,
    gate_input,
    step_raw,
    step_bias,
    decay_log,
    skip_gain,
    conv_head,
    conv_state,
    norm_gain,
    next_weight,
):
    token_count = head_input.shape[1]
    local_width = head_input.shape[2]
    head_count = step_raw.shape[1]
    head_width = local_width // head_count
    block_count = token_count // BLOCK
    part = weight_part(copied(next_weight[0]))
    tails = last_positions(head_input[0], state_proj[0])
    behind = from_behind(tails, CTX, 1)
    step_size = jax.nn.softplus(step_raw[0] + step_bias[0][:, None])
    log_decay = -jnp.exp(decay_log[0])[:, None] * step_size
    blocks_step = step_size.reshape(head_count, block_count, BLOCK)
    blocks_decay = log_decay.reshape(head_count, block_count, BLOCK)
    offset = jnp.zeros((), jnp.int32)
    lower_tri = causal(offset).astype(jnp.float32)
    cumulative = jnp.einsum("hcs,ts->hct", blocks_decay, lower_tri, precision=HIGHEST)
    tail_weight = jnp.exp(cumulative[..., -1:] - cumulative) * blocks_step
    wide, narrow, wide_taps, narrow_taps = loaded(
        head_input[0], state_proj[0], conv_head[0], conv_state[0]
    )
    conv_xt, conv_bc, sent = prepared(
        wide,
        narrow,
        behind,
        wide_taps,
        narrow_taps,
        tail_weight[:, 0],
        cumulative[:, 0, -1],
        CTX,
    )
    full_weight = gathered_weight(part)
    prior = scanned_slices(sent, CTX)
    prior, conv_xt, conv_bc, gate_input, offset = lax.optimization_barrier(
        (prior, conv_xt, conv_bc, gate_input, offset)
    )
    prior_state = lax.all_to_all(prior, CTX, 0, 0, tiled=True).reshape(
        head_count, head_width, STATE
    )
    causal_mask = causal(offset)
    blocks_x = conv_xt.T.reshape(block_count, BLOCK, head_count, head_width)
    blocks_b = conv_bc[:, :STATE].reshape(block_count, BLOCK, STATE)
    blocks_c = conv_bc[:, STATE:].reshape(block_count, BLOCK, STATE)
    scores = jnp.einsum("ctn,csn->cts", blocks_c, blocks_b, preferred_element_type=jnp.float32)
    decay_diff = jnp.where(causal_mask, cumulative[..., :, None] - cumulative[..., None, :], 0.0)
    mix_weight = jnp.where(
        causal_mask, scores[None] * jnp.exp(decay_diff) * blocks_step[:, :, None, :], 0.0
    ).astype(jnp.bfloat16)
    intra_part = jnp.einsum(
        "hcts,cshp->cthp", mix_weight, blocks_x, preferred_element_type=jnp.float32
    )
    local_part = intra_part + skip_gain[0][None, None, :, None] * blocks_x.astype(jnp.float32)
    gate = jax.nn.silu(gate_input[0].astype(jnp.float32))
    local_part, gate = lax.optimization_barrier((local_part, gate))
    inter_part = (
        jnp.einsum("ctn,hpn->cthp", blocks_c, prior_state, preferred_element_type=jnp.float32)
        * jnp.exp(cumulative).transpose(1, 2, 0)[..., None]
    )
    gated = (local_part + inter_part).reshape(token_count, local_width) * gate
    high, low = split_in_two(jnp.sum(gated * gated, axis=1))
    extra = jnp.stack([high, low] + [jnp.zeros_like(high)] * (EXTRA - 2), axis=1)
    features = (gated * norm_gain[0][None]).astype(jnp.bfloat16)
    arrived = shifted(jnp.concatenate([features, extra], axis=1), "section", 1)
    other = other_half(arrived, "mp")
    features, scale = assembled(arrived.T, other.T, "mp")
    return projected(features, scale, full_weight)[None]


def solution(mesh):
    finer = Mesh(
        mesh.devices.reshape(mesh.shape["section"], 8, 8, mesh.shape["mp"]),
        ("section", "ctx_0", "ctx_1", "mp"),
    )
    in_specs = (
        P("section", CTX, "mp"),
        P("section", CTX, None),
        P("section", CTX, "mp"),
        P("section", "mp", CTX),
        P("section", "mp"),
        P("section", "mp"),
        P("section", "mp"),
        P("section", None, "mp"),
        P("section", None, None),
        P("section", "mp"),
        P("section", CTX, "mp"),
    )
    out_specs = P("section", CTX, "mp")
    return jax.shard_map(
        section_block, mesh=finer, in_specs=in_specs, out_specs=out_specs, check_vma=False
    )
```
